32 devices in a mesh: rep: 2 (over z, core), dp: 16 (over x, y).
Axes of the slice: x: 4, y: 4, z: 1, core: 2. Of those that a mesh axis runs over, the one named last changes fastest.
The devices are a block of a 4x4x8 slice.
Arguments:
- g_w_gate: bfloat16 [32, 2, 1024, 3200], P(('rep', 'dp')), parts along dimension 0
- g_w_up: bfloat16 [32, 2, 1024, 3200], P(('rep', 'dp')), parts along dimension 0
- g_w_down: bfloat16 [32, 2, 3200, 1024], P(('rep', 'dp')), parts along dimension 0
- w_gate: bfloat16 [2, 1024, 3200], replicated
- w_up: bfloat16 [2, 1024, 3200], replicated
- w_down: bfloat16 [2, 3200, 1024], replicated
- m_w_gate: float32 [2, 1024, 3200], P(None, 'dp')
- m_w_up: float32 [2, 1024, 3200], P(None, 'dp')
- m_w_down: float32 [2, 3200, 1024], P(None, 'dp')
- v_w_gate: float32 [2, 1024, 3200], P(None, 'dp')
- v_w_up: float32 [2, 1024, 3200], P(None, 'dp')
- v_w_down: float32 [2, 3200, 1024], P(None, 'dp')
Outputs:
- output 1: bfloat16 [4, 1024, 3200], P('rep'), parts along dimension 0
- output 2: bfloat16 [4, 1024, 3200], P('rep'), parts along dimension 0
- output 3: bfloat16 [4, 3200, 1024], P('rep'), parts along dimension 0
- output 4: float32 [4, 1024, 3200], P('rep', 'dp'), parts along dimension 0
- output 5: float32 [4, 1024, 3200], P('rep', 'dp'), parts along dimension 0
- output 6: float32 [4, 3200, 1024], P('rep', 'dp'), parts along dimension 0
- output 7: float32 [4, 1024, 3200], P('rep', 'dp'), parts along dimension 0
- output 8: float32 [4, 1024, 3200], P('rep', 'dp'), parts along dimension 0
- output 9: float32 [4, 3200, 1024], P('rep', 'dp'), parts along dimension 0
There are 2 independent parts. The reference program is written for one: setup_inputs(seed, part) draws one part's arguments, and reference() takes and returns one part's arrays. A program takes and returns all parts, laid end to end along the dimension named above; an argument that names none is the same for every part.
All inputs are finite; a program needn't handle non-finite values.
Results may differ from the reference program's by a relative error of at most 0.022.
Values are sent between devices in bfloat16 or wider.
A program may use at most 768 MiB of HBM per device.

```python
import jax
import jax.numpy as jnp
from jax import lax

DEVICES = 16
D = 1024
FF = 3200
LAYERS = 2
NAMES = ("w_gate", "w_up", "w_down")
SHAPES = {"w_gate": (LAYERS, D, FF), "w_up": (LAYERS, D, FF), "w_down": (LAYERS, FF, D)}


def setup_inputs(seed: int = 0, part: int = 0) -> dict:
    kz, *keys = jax.random.split(jax.random.key(seed), 1 + 5 * len(NAMES))
    loud = 2.0 ** jax.random.uniform(kz, (), jnp.float32, -1.0, 1.0)
    drawn = {}
    for name, key, both in zip(NAMES, keys[:3], keys[3:6], strict=True):
        own = jax.random.normal(jax.random.fold_in(key, part), (DEVICES, *SHAPES[name]), jnp.float32)
        shared = jax.random.normal(jax.random.fold_in(both, part), SHAPES[name], jnp.float32)
        drawn["g_" + name] = (loud * (0.7 * shared / DEVICES + 0.7 * own * DEVICES**-0.5)).astype(jnp.bfloat16)
    for name, key in zip(NAMES, keys[6:9], strict=True):
        drawn[name] = (jax.random.normal(key, SHAPES[name], jnp.float32) * SHAPES[name][1] ** -0.5).astype(jnp.bfloat16)
    for name, key in zip(NAMES, keys[9:12], strict=True):
        drawn["m_" + name] = loud * 0.5 * jax.random.normal(key, SHAPES[name], jnp.float32)
    for name, key in zip(NAMES, keys[12:15], strict=True):
        drawn["v_" + name] = loud * loud * jax.random.uniform(key, SHAPES[name], jnp.float32, 0.5, 1.5)
    return drawn


def adamw(w, m, v, g):
    m = 0.9 * m + 0.1 * g
    v = 0.95 * v + 0.05 * g * g
    step = m * lax.rsqrt(v + 1e-8) + 0.1 * w
    return (w - 0.02 * step).astype(jnp.bfloat16), m, v


def reference(g_w_gate, g_w_up, g_w_down, w_gate, w_up, w_down, m_w_gate, m_w_up, m_w_down, v_w_gate, v_w_up, v_w_down):
    def total(terms):
        return lax.scan(lambda so_far, term: (so_far + term.astype(jnp.float32), None), jnp.zeros(terms.shape[1:], jnp.float32), terms)[0]

    gradients = [total(terms).astype(jnp.bfloat16).astype(jnp.float32) for terms in (g_w_gate, g_w_up, g_w_down)]
    new = [
        adamw(w.astype(jnp.float32), m, v, g)
        for w, m, v, g in zip((w_gate, w_up, w_down), (m_w_gate, m_w_up, m_w_down), (v_w_gate, v_w_up, v_w_down), gradients, strict=True)
    ]
    return tuple(one[which] for which in range(3) for one in new)
```

```python
import functools
import math

import jax
import jax.numpy as jnp
from jax import lax
from jax.experimental import pallas as pl
from jax.experimental.pallas import tpu as pltpu
from jax.sharding import PartitionSpec as P

MESH = pl.DeviceIdType.MESH
S1, S2A, S2B, T1, T2A, T2B, A1, A1F, A2, A2F = range(10)
KINDS = 10
STAGES = 9


def halves(shape):
    rows, columns = shape
    if rows % 32 == 0:
        return (rows // 4, columns), lambda i, n=1: (pl.ds(i * (rows // 4), n * (rows // 4)), slice(None))
    return (rows, columns // 4), lambda i, n=1: (slice(None), pl.ds(i * (columns // 4), n * (columns // 4)))


def pieces(shape):
    rows, columns = shape
    if rows <= 64:
        n = next(k for k in (5, 3, 2, 1) if columns % (k * 128) == 0)
        return n, lambda i: (slice(None), pl.ds(pl.multiple_of(i * (columns // n), 128), columns // n))
    n = next(k for k in (5, 4, 2, 1) if rows % (k * 8) == 0)
    return n, lambda i: (pl.ds(pl.multiple_of(i * (rows // n), 8), rows // n), slice(None))


def kernel(side, layers, shapes, *refs):
    n = len(shapes)
    gs, ws, ms, vs, outs, gouts = (refs[i * n : (i + 1) * n] for i in range(6))
    scratch = refs[6 * n : -4]
    send, recv, local, stored = refs[-4:]
    kinds = list(dict.fromkeys(shapes))
    per = len(scratch) // len(kinds)
    held = {shape: scratch[i * per : (i + 1) * per] for i, shape in enumerate(kinds)}
    jobs, seen = [], {shape: 0 for shape in kinds}
    for which, shape in enumerate(shapes):
        for layer in range(layers):
            jobs.append((which, layer, shape, seen[shape]))
            seen[shape] += 1

    me = lax.axis_index("dp")
    xy = (lax.div(me, side), lax.rem(me, side))

    def at(i, by):
        return lax.rem(i + (by + side), side)

    def place(c):
        return xy[c], xy[1 - c]

    def pair(c, p, s):
        return (p, s) if c == 0 else (s, p)

    def device(c, p, s):
        a, b = pair(c, p, s)
        return {"dp": a * side + b}

    signs = (1, -1)
    barrier = pltpu.get_barrier_semaphore()
    for c in range(2):
        p, s = place(c)
        for by in signs:
            pl.semaphore_signal(barrier, inc=1, device_id=device(c, at(p, by), s), device_id_type=MESH)
    pl.semaphore_wait(barrier, 4)

    def copy(q, c, d, kind):
        which, layer, shape, slot = jobs[q]
        r1, r2, q1, q2, oc, ob, mb, vb, wb, wn = held[shape]
        quarter, index = halves(shape)
        g, out = gs[which], outs[which]
        p, s = place(c)
        by = signs[d]

        def chunk(i, h):
            return g.at[(layer, i, slice(None), *index(2 * c + h))] if c == 0 else g.at[(layer, slice(None), i, *index(2 * c + h))]

        def block(i, j, h=0, width=2):
            return out.at[(layer, *pair(c, i, j), *index(2 * c + h, width))]

        def row(i, h=0, width=2):
            return block(i, slice(None), h, width)

        along = device(c, at(p, by), s)
        across = device(c, p, at(s, by))
        if kind == S1:
            src, dst, to = chunk(at(p, 2), d), r1.at[slot, c, d], along
        elif kind == S2A:
            src, dst, to = chunk(at(p, by), 1 - d), r2.at[slot, c, d, 1 - d], along
        elif kind == S2B:
            src, dst, to = r1.at[slot, c, d], r2.at[slot, c, d, d], along
        elif kind == T1:
            src, dst, to = oc.at[slot, c, d, at(s, 2)], q1.at[slot, c, d], across
        elif kind == T2A:
            src, dst, to = oc.at[slot, c, 1 - d, at(s, by)], q2.at[slot, c, d, 1 - d], across
        elif kind == T2B:
            src, dst, to = q1.at[slot, c, d], q2.at[slot, c, d, d], across
        elif kind == A1:
            src, dst, to = wn.at[slot, c], block(p, s), across
        elif kind == A1F:
            src, dst, to = block(p, at(s, -by), d, 1), block(p, at(s, -by), d, 1), across
        elif kind == A2:
            src, dst, to = row(p), row(p), along
        else:
            src, dst, to = row(at(p, -by), d, 1), row(at(p, -by), d, 1), along
        return pltpu.make_async_remote_copy(
            src_ref=src,
            dst_ref=dst,
            send_sem=send.at[q, c, d, kind],
            recv_sem=recv.at[q, c, d, kind],
            device_id=to,
            device_id_type=MESH,
        )

    each = [(c, d) for c in range(2) for d in range(2)]

    def start(q, kind):
        for c, d in each:
            copy(q, c, d, kind).start()

    def arrived(q, kind):
        for c, d in each:
            copy(q, c, d, kind).wait_recv()

    def own(q, c, d, kept):
        which, layer, shape, slot = jobs[q]
        oc, ob = held[shape][4:6]
        _, index = halves(shape)
        p, _ = place(c)
        g = gs[which]

        def chunk(i, h):
            return g.at[(layer, i, slice(None), *index(2 * c + h))] if c == 0 else g.at[(layer, slice(None), i, *index(2 * c + h))]

        if kept:
            return pltpu.make_async_copy(chunk(p, d), oc.at[slot, c, d], local.at[q, 4 + 2 * c + d])
        return pltpu.make_async_copy(chunk(at(p, signs[d]), d), ob.at[slot % 2, c, d], local.at[q, 2 * c + d])

    def state(q):
        which, layer, shape, slot = jobs[q]
        mb, vb, wb = held[shape][6:9]
        sources = (ms[which].at[layer], vs[which].at[layer], ws[which].at[layer, xy[0], xy[1]])
        return [
            pltpu.make_async_copy(src, buffer.at[slot % 2], local.at[q, 8 + i])
            for i, (src, buffer) in enumerate(zip(sources, (mb, vb, wb), strict=True))
        ]

    def weight(q, c):
        which, layer, shape, slot = jobs[q]
        mine = outs[which].at[(layer, xy[0], xy[1], *halves(shape)[1](2 * c, 2))]
        return pltpu.make_async_copy(held[shape][9].at[slot, c], mine, stored.at[q, c, 2])

    def gradient(q, c, h):
        which, layer, shape, slot = jobs[q]
        mine = gouts[which].at[(layer, *halves(shape)[1](2 * c + h))]
        return pltpu.make_async_copy(held[shape][3].at[slot, c, 0, h], mine, stored.at[q, c, h])

    def walk(shape, body):
        steps, piece = pieces(halves(shape)[0])

        @pl.loop(0, steps)
        def _(i):
            body(piece(i))

    def add(shape, *todo):
        def body(where):
            for (ref, lead), terms in todo:
                parts = [t[(*at_, *where)].astype(jnp.float32) for t, at_ in terms]
                ref[(*lead, *where)] = functools.reduce(lambda a, b: a + b, parts).astype(ref.dtype)

        walk(shape, body)

    def stage(k, q):
        which, layer, shape, slot = jobs[q]
        r1, r2, q1, q2, oc, ob, mb, vb, wb, wn = held[shape]
        _, index = halves(shape)
        if k == 0:
            start(q, S1)
            start(q, S2A)
            for c, d in each:
                own(q, c, d, False).start()
                own(q, c, d, True).start()
        elif k == 1:
            for c, d in each:
                copy(q, c, d, S1).wait_recv()
                own(q, c, d, False).wait()

                @pl.loop(0, side)
                def _(j, c=c, d=d):
                    there = (slot, c, d, j)
                    add(shape, ((r1, there), ((r1, there), (ob, (slot % 2, c, d, j)))))

                copy(q, c, d, S2B).start()
        elif k == 2:
            arrived(q, S2A)
            arrived(q, S2B)
            for c, d in each:
                own(q, c, d, True).wait()
            for c in range(2):
                s = place(c)[1]
                for h, j in ((0, at(s, 2)), (1, at(s, 2)), (1, at(s, 1)), (0, at(s, -1))):
                    here = (slot, c, h, j)
                    add(shape, ((oc, here), ((oc, here), (r2, (slot, c, 0, h, j)), (r2, (slot, c, 1, h, j)))))
            start(q, T1)
            start(q, T2A)
        elif k == 3:
            for one in state(q):
                one.start()
            for c, d in each:
                s = place(c)[1]
                copy(q, c, d, T1).wait_recv()
                j = at(s, signs[d])
                here = (slot, c, d)
                add(shape, ((q1, here), ((oc, (*here, j)), (r2, (slot, c, 0, d, j)), (r2, (slot, c, 1, d, j)), (q1, here))))
                copy(q, c, d, T2B).start()
        elif k == 4:
            arrived(q, T2A)
            arrived(q, T2B)
            for one in state(q):
                one.wait()
            for c in range(2):
                s = place(c)[1]
                for h in range(2):
                    terms = [(oc, (slot, c, h, s))] + [(r2, (slot, c, d, h, s)) for d in range(2)] + [(q2, (slot, c, d, h)) for d in range(2)]
                    quarter = index(2 * c + h)
                    offsets = [x.start if isinstance(x, pl.Slice) else 0 for x in quarter]
                    half = [x.start if isinstance(x, pl.Slice) else 0 for x in index(h)]

                    def body(where, c=c, h=h, terms=terms, offsets=offsets, half=half):
                        def shifted(by):
                            full = []
                            for w, size, o in zip(where, halves(shape)[0], by, strict=True):
                                full.append(pl.ds(o, size) if isinstance(w, slice) else pl.ds(o + w.start, w.size))
                            return tuple(full)

                        g = functools.reduce(lambda a, b: a + b, [t[(*lead, *where)].astype(jnp.float32) for t, lead in terms])
                        g16 = g.astype(jnp.bfloat16)
                        g = g16.astype(jnp.float32)
                        q2[(slot, c, 0, h, *where)] = g16
                        there = (slot % 2, *shifted(offsets))
                        w = wb[there].astype(jnp.float32)
                        m = 0.9 * mb[there] + 0.1 * g
                        v = 0.95 * vb[there] + 0.05 * g * g
                        new = w - 0.02 * (m * lax.rsqrt(v + 1e-8) + 0.1 * w)
                        wn[(slot, c, *shifted(half))] = new.astype(jnp.bfloat16)

                    walk(shape, body)
                for d in range(2):
                    copy(q, c, d, A1).start()
                weight(q, c).start()
                for h in range(2):
                    gradient(q, c, h).start()
        elif k == 5:
            arrived(q, A1)
            start(q, A1F)
        elif k == 6:
            for c in range(2):
                weight(q, c).wait()
            arrived(q, A1F)
            start(q, A2)
        elif k == 7:
            arrived(q, A2)
            start(q, A2F)
        else:
            arrived(q, A2F)

    for t in range(len(jobs) + STAGES - 1):
        for k in range(STAGES):
            if 0 <= t - k < len(jobs):
                stage(k, t - k)

    for q in range(len(jobs)):
        for c in range(2):
            for h in range(2):
                gradient(q, c, h).wait()
        for kind in range(KINDS):
            for c, d in each:
                copy(q, c, d, kind).wait_send()


def step_kernel(side, layers, shapes, terms, weights, m, v):
    scratch = []
    for shape in dict.fromkeys(shapes):
        count = layers * shapes.count(shape)
        quarter, _ = halves(shape)
        both = (quarter[0] * 2, quarter[1]) if quarter[1] == shape[1] else (quarter[0], quarter[1] * 2)
        scratch += [
            pltpu.VMEM((count, 2, 2, side, *quarter), jnp.bfloat16),
            pltpu.VMEM((count, 2, 2, 2, side, *quarter), jnp.bfloat16),
            pltpu.VMEM((count, 2, 2, *quarter), jnp.bfloat16),
            pltpu.VMEM((count, 2, 2, 2, *quarter), jnp.bfloat16),
            pltpu.VMEM((count, 2, 2, side, *quarter), jnp.bfloat16),
            pltpu.VMEM((2, 2, 2, side, *quarter), jnp.bfloat16),
            pltpu.VMEM((2, *shape), jnp.float32),
            pltpu.VMEM((2, *shape), jnp.float32),
            pltpu.VMEM((2, *shape), jnp.bfloat16),
            pltpu.VMEM((count, 2, *both), jnp.bfloat16),
        ]
    jobs = layers * len(shapes)
    anywhere = pl.BlockSpec(memory_space=pl.ANY)
    return pl.pallas_call(
        functools.partial(kernel, side, layers, shapes),
        out_shape=[jax.ShapeDtypeStruct(w.shape, jnp.bfloat16) for w in weights]
        + [jax.ShapeDtypeStruct(one.shape, jnp.bfloat16) for one in m],
        in_specs=[anywhere] * (4 * len(shapes)),
        out_specs=[anywhere] * (2 * len(shapes)),
        scratch_shapes=scratch
        + [
            pltpu.SemaphoreType.DMA((jobs, 2, 2, KINDS)),
            pltpu.SemaphoreType.DMA((jobs, 2, 2, KINDS)),
            pltpu.SemaphoreType.DMA((jobs, 11)),
            pltpu.SemaphoreType.DMA((jobs, 2, 3)),
        ],
        compiler_params=pltpu.CompilerParams(collective_id=0, has_side_effects=True, vmem_limit_bytes=67_043_328),
        name="step",
    )(*terms, *weights, *m, *v)


def solution(mesh):
    side = math.isqrt(mesh.shape["dp"])

    def step(*arrays):
        terms, weights, m, v = (arrays[i : i + 3] for i in (0, 3, 6, 9))
        shapes = tuple(one.shape[1:] for one in m)
        layers = m[0].shape[0]
        split = [(layers, side, side, *shape) for shape in shapes]
        *new, g0, g1, g2 = step_kernel(
            side,
            layers,
            shapes,
            [t[0].reshape(s) for t, s in zip(terms, split, strict=True)],
            [w.reshape(s) for w, s in zip(weights, split, strict=True)],
            m,
            v,
        )
        whole = [one.reshape(w.shape) for one, w in zip(new, weights, strict=True)]
        g = [one.astype(jnp.float32) for one in (g0, g1, g2)]
        return (
            *whole,
            *(0.9 * a + 0.1 * b for a, b in zip(m, g, strict=True)),
            *(0.95 * a + 0.05 * b * b for a, b in zip(v, g, strict=True)),
        )

    all_of, cut = P(None, None, None), P(None, "dp", None)
    return jax.shard_map(
        step,
        mesh=mesh,
        in_specs=(P(("rep", "dp"), None, None, None),) * 3 + (all_of,) * 3 + (cut,) * 6,
        out_specs=(P("rep", None, None),) * 3 + (P("rep", "dp", None),) * 6,
        check_vma=False,
    )
```

```python
import functools
import math

import jax
import jax.numpy as jnp
from jax import lax
from jax.experimental import pallas as pl
from jax.experimental.pallas import tpu as pltpu
from jax.sharding import PartitionSpec as P

MESH = pl.DeviceIdType.MESH
S1, S2A, S2B, T1, T2A, T2B, A1, A1F, A2, A2F = range(10)
KINDS = 10
STAGES = 9
SLOTS, SLOTS_F = 8, 4


def halves(shape):
    rows, columns = shape
    if rows % 32 == 0:
        return (rows // 4, columns), lambda i, n=1: (pl.ds(i * (rows // 4), n * (rows // 4)), slice(None))
    return (rows, columns // 4), lambda i, n=1: (slice(None), pl.ds(i * (columns // 4), n * (columns // 4)))


def pieces(shape):
    rows, columns = shape
    if rows <= 64:
        n = next(k for k in (5, 3, 2, 1) if columns % (k * 128) == 0)
        return n, lambda i: (slice(None), pl.ds(pl.multiple_of(i * (columns // n), 128), columns // n))
    n = next(k for k in (5, 4, 2, 1) if rows % (k * 8) == 0)
    return n, lambda i: (pl.ds(pl.multiple_of(i * (rows // n), 8), rows // n), slice(None))


def kernel(side, layers, shapes, late, *refs):
    n = len(shapes)
    gs, ws, ms, vs, outs, mouts, vouts = (refs[i * n : (i + 1) * n] for i in range(7))
    passed = refs[7 * n : 7 * n + 4]
    scratch = refs[7 * n + 4 : -4]
    send, recv, local, stored = refs[-4:]
    kinds = list(dict.fromkeys(shapes))
    per = len(scratch) // len(kinds)
    held = {shape: scratch[i * per : (i + 1) * per] for i, shape in enumerate(kinds)}
    jobs, seen = [], {shape: 0 for shape in kinds}
    for which in sorted(range(n), key=lambda i: i in late):
        for layer in range(layers):
            jobs.append((which, layer, shapes[which], seen[shapes[which]]))
            seen[shapes[which]] += 1
    first_late = len(jobs) - layers * len(late)

    me = lax.axis_index("dp")
    xy = (lax.div(me, side), lax.rem(me, side))

    def at(i, by):
        return lax.rem(i + (by + side), side)

    def place(c):
        return xy[c], xy[1 - c]

    def pair(c, p, s):
        return (p, s) if c == 0 else (s, p)

    def device(c, p, s):
        a, b = pair(c, p, s)
        return {"dp": a * side + b}

    signs = (1, -1)
    barrier = pltpu.get_barrier_semaphore()
    for c in range(2):
        p, s = place(c)
        for by in signs:
            pl.semaphore_signal(barrier, inc=1, device_id=device(c, at(p, by), s), device_id_type=MESH)
    pl.semaphore_wait(barrier, 4)

    def copy(q, c, d, kind):
        which, layer, shape, slot = jobs[q]
        r1, r2, q1, q2, oc, ob, mb, vb, wb, wn = held[shape]
        quarter, index = halves(shape)
        g, out = gs[which], outs[which]
        p, s = place(c)
        by = signs[d]

        def chunk(i, h):
            return g.at[(layer, i, slice(None), *index(2 * c + h))] if c == 0 else g.at[(layer, slice(None), i, *index(2 * c + h))]

        def block(i, j, h=0, width=2):
            return out.at[(layer, *pair(c, i, j), *index(2 * c + h, width))]

        def row(i, h=0, width=2):
            return block(i, slice(None), h, width)

        along = device(c, at(p, by), s)
        across = device(c, p, at(s, by))
        if kind == S1:
            src, dst, to = chunk(at(p, 2), d), r1.at[slot, c, d], along
        elif kind == S2A:
            src, dst, to = chunk(at(p, by), 1 - d), r2.at[slot, c, d, 1 - d], along
        elif kind == S2B:
            src, dst, to = r1.at[slot, c, d], r2.at[slot, c, d, d], along
        elif kind == T1:
            src, dst, to = oc.at[slot, c, d, at(s, 2)], q1.at[slot, c, d], across
        elif kind == T2A:
            src, dst, to = oc.at[slot, c, 1 - d, at(s, by)], q2.at[slot, c, d, 1 - d], across
        elif kind == T2B:
            src, dst, to = q1.at[slot, c, d], q2.at[slot, c, d, d], across
        elif kind == A1:
            src, dst, to = wn.at[slot, c], block(p, s), across
        elif kind == A1F:
            src, dst, to = block(p, at(s, -by), d, 1), block(p, at(s, -by), d, 1), across
        elif kind == A2 and q >= first_late:
            src, dst, to = row(p, 1 - d, 1), row(p, 1 - d, 1), along
        elif q >= first_late:
            src, dst, to = row(p, d, 1), passed[2 * c + d].at[q - first_late], along
        elif kind == A2:
            src, dst, to = row(p), row(p), along
        else:
            src, dst, to = row(at(p, -by), d, 1), row(at(p, -by), d, 1), along
        return pltpu.make_async_remote_copy(
            src_ref=src,
            dst_ref=dst,
            send_sem=send.at[q, c, d, kind],
            recv_sem=recv.at[q, c, d, kind],
            device_id=to,
            device_id_type=MESH,
        )

    each = [(c, d) for c in range(2) for d in range(2)]

    def start(q, kind):
        for c, d in each:
            copy(q, c, d, kind).start()

    def arrived(q, kind):
        for c, d in each:
            copy(q, c, d, kind).wait_recv()

    def own(q, c, d, kept):
        which, layer, shape, slot = jobs[q]
        oc, ob = held[shape][4:6]
        _, index = halves(shape)
        p, _ = place(c)
        g = gs[which]

        def chunk(i, h):
            return g.at[(layer, i, slice(None), *index(2 * c + h))] if c == 0 else g.at[(layer, slice(None), i, *index(2 * c + h))]

        if kept:
            return pltpu.make_async_copy(chunk(p, d), oc.at[slot, c, d], local.at[q, 4 + 2 * c + d])
        return pltpu.make_async_copy(chunk(at(p, signs[d]), d), ob.at[slot % 2, c, d], local.at[q, 2 * c + d])

    def state(q):
        which, layer, shape, slot = jobs[q]
        mb, vb, wb = held[shape][6:9]
        sources = (ms[which].at[layer], vs[which].at[layer], ws[which].at[layer, xy[0], xy[1]])
        return [
            pltpu.make_async_copy(src, buffer.at[slot % 2], local.at[q, 8 + i])
            for i, (src, buffer) in enumerate(zip(sources, (mb, vb, wb), strict=True))
        ]

    def weight(q, c):
        which, layer, shape, slot = jobs[q]
        mine = outs[which].at[(layer, xy[0], xy[1], *halves(shape)[1](2 * c, 2))]
        return pltpu.make_async_copy(held[shape][9].at[slot, c], mine, stored.at[q, c, 2])

    def moments(q):
        which, layer, shape, slot = jobs[q]
        return [
            pltpu.make_async_copy(buffer.at[slot % 2], out[which].at[layer], stored.at[q, i, 0])
            for i, (buffer, out) in enumerate(zip(held[shape][6:8], (mouts, vouts), strict=True))
        ]

    def walk(shape, body):
        steps, piece = pieces(halves(shape)[0])

        @pl.loop(0, steps)
        def _(i):
            body(piece(i))

    def add(shape, *todo):
        def body(where):
            for (ref, lead), terms in todo:
                parts = [t[(*at_, *where)].astype(jnp.float32) for t, at_ in terms]
                ref[(*lead, *where)] = functools.reduce(lambda a, b: a + b, parts).astype(ref.dtype)

        walk(shape, body)

    def stage(k, q):
        which, layer, shape, slot = jobs[q]
        r1, r2, q1, q2, oc, ob, mb, vb, wb, wn = held[shape]
        _, index = halves(shape)
        if k == 0:
            start(q, S1)
            start(q, S2A)
            for c, d in each:
                own(q, c, d, False).start()
                own(q, c, d, True).start()
        elif k == 1:
            for c, d in each:
                copy(q, c, d, S1).wait_recv()
                own(q, c, d, False).wait()

                @pl.loop(0, side)
                def _(j, c=c, d=d):
                    there = (slot, c, d, j)
                    add(shape, ((r1, there), ((r1, there), (ob, (slot % 2, c, d, j)))))

                copy(q, c, d, S2B).start()
        elif k == 2:
            arrived(q, S2A)
            arrived(q, S2B)
            for c, d in each:
                own(q, c, d, True).wait()
            for c in range(2):
                s = place(c)[1]
                for h, j in ((0, at(s, 2)), (1, at(s, 2)), (1, at(s, 1)), (0, at(s, -1))):
                    here = (slot, c, h, j)
                    add(shape, ((oc, here), ((oc, here), (r2, (slot, c, 0, h, j)), (r2, (slot, c, 1, h, j)))))
            start(q, T1)
            start(q, T2A)
        elif k == 3:
            if slot >= 2:
                for one in moments(next(i for i, job in enumerate(jobs) if job[2:] == (shape, slot - 2))):
                    one.wait()
            for one in state(q):
                one.start()
            for c, d in each:
                s = place(c)[1]
                copy(q, c, d, T1).wait_recv()
                j = at(s, signs[d])
                here = (slot, c, d)
                add(shape, ((q1, here), ((oc, (*here, j)), (r2, (slot, c, 0, d, j)), (r2, (slot, c, 1, d, j)), (q1, here))))
                copy(q, c, d, T2B).start()
        elif k == 4:
            arrived(q, T2A)
            arrived(q, T2B)
            for one in state(q):
                one.wait()
            for c in range(2):
                s = place(c)[1]
                for h in range(2):
                    terms = [(oc, (slot, c, h, s))] + [(r2, (slot, c, d, h, s)) for d in range(2)] + [(q2, (slot, c, d, h)) for d in range(2)]
                    quarter = index(2 * c + h)
                    offsets = [x.start if isinstance(x, pl.Slice) else 0 for x in quarter]
                    half = [x.start if isinstance(x, pl.Slice) else 0 for x in index(h)]

                    def body(where, c=c, h=h, terms=terms, offsets=offsets, half=half):
                        def shifted(by):
                            full = []
                            for w, size, o in zip(where, halves(shape)[0], by, strict=True):
                                full.append(pl.ds(o, size) if isinstance(w, slice) else pl.ds(o + w.start, w.size))
                            return tuple(full)

                        g = functools.reduce(lambda a, b: a + b, [t[(*lead, *where)].astype(jnp.float32) for t, lead in terms])
                        g = g.astype(jnp.bfloat16).astype(jnp.float32)
                        there = (slot % 2, *shifted(offsets))
                        w = wb[there].astype(jnp.float32)
                        m = 0.9 * mb[there] + 0.1 * g
                        v = 0.95 * vb[there] + 0.05 * g * g
                        mb[there] = m
                        vb[there] = v
                        new = w - 0.02 * (m * lax.rsqrt(v + 1e-8) + 0.1 * w)
                        wn[(slot, c, *shifted(half))] = new.astype(jnp.bfloat16)

                    walk(shape, body)
                for d in range(2):
                    copy(q, c, d, A1).start()
                weight(q, c).start()
            for one in moments(q):
                one.start()
        elif k == 5:
            arrived(q, A1)
            start(q, A1F)
        elif k == 6:
            for c in range(2):
                weight(q, c).wait()
            arrived(q, A1F)
            if q >= first_late:
                start(q, A2F)
            start(q, A2)
        elif k == 7:
            arrived(q, A2)
            if q < first_late:
                start(q, A2F)
        else:
            arrived(q, A2F)

    for t in range(len(jobs) + STAGES - 1):
        for k in range(STAGES):
            if 0 <= t - k < len(jobs):
                stage(k, t - k)

    for q, (_, _, shape, slot) in enumerate(jobs):
        if slot + 2 >= seen[shape]:
            for one in moments(q):
                one.wait()
        for kind in range(KINDS):
            for c, d in each:
                copy(q, c, d, kind).wait_send()


def step_kernel(side, layers, shapes, late, terms, weights, m, v):
    scratch = []
    for shape in dict.fromkeys(shapes):
        count = layers * shapes.count(shape)
        quarter, _ = halves(shape)
        both = (quarter[0] * 2, quarter[1]) if quarter[1] == shape[1] else (quarter[0], quarter[1] * 2)
        scratch += [
            pltpu.VMEM((count, 2, 2, side, *quarter), jnp.bfloat16),
            pltpu.VMEM((count, 2, 2, 2, side, *quarter), jnp.bfloat16),
            pltpu.VMEM((count, 2, 2, *quarter), jnp.bfloat16),
            pltpu.VMEM((count, 2, 2, 2, *quarter), jnp.bfloat16),
            pltpu.VMEM((count, 2, 2, side, *quarter), jnp.bfloat16),
            pltpu.VMEM((2, 2, 2, side, *quarter), jnp.bfloat16),
            pltpu.VMEM((2, *shape), jnp.float32),
            pltpu.VMEM((2, *shape), jnp.float32),
            pltpu.VMEM((2, *shape), jnp.bfloat16),
            pltpu.VMEM((count, 2, *both), jnp.bfloat16),
        ]
    jobs = layers * len(shapes)
    passed = (layers * len(late), side, *halves(shapes[late[0]])[0])
    anywhere = pl.BlockSpec(memory_space=pl.ANY)
    outs = pl.pallas_call(
        functools.partial(kernel, side, layers, shapes, late),
        out_shape=[jax.ShapeDtypeStruct(w.shape, jnp.bfloat16) for w in weights]
        + [jax.ShapeDtypeStruct(one.shape, jnp.float32) for one in (*m, *v)]
        + [jax.ShapeDtypeStruct(passed, jnp.bfloat16)] * 4,
        in_specs=[anywhere] * (4 * len(shapes)),
        out_specs=[anywhere] * (3 * len(shapes) + 4),
        scratch_shapes=scratch
        + [
            pltpu.SemaphoreType.DMA((jobs, 2, 2, KINDS)),
            pltpu.SemaphoreType.DMA((jobs, 2, 2, KINDS)),
            pltpu.SemaphoreType.DMA((jobs, 11)),
            pltpu.SemaphoreType.DMA((jobs, 2, 3)),
        ],
        compiler_params=pltpu.CompilerParams(collective_id=0, has_side_effects=True, vmem_limit_bytes=67_043_328),
        name="step",
    )(*terms, *weights, *m, *v)
    return outs[:-4], outs[-4:]


def move(moves, slots, sems):
    inward, outward = sems
    used = {}
    plan = []
    for i, (src, dst, name) in enumerate(moves):
        buffer = slots[name]
        turn = used.setdefault(name, [])
        place = buffer.at[len(turn) % buffer.shape[0]]
        before = turn[-buffer.shape[0]] if len(turn) >= buffer.shape[0] else None
        turn.append(i)
        plan.append((functools.partial(pltpu.make_async_copy, src, place, inward.at[i]), functools.partial(pltpu.make_async_copy, place, dst, outward.at[i]), before))
    done = set()
    ahead = 0
    for i in range(len(plan)):
        while ahead < len(plan) and (plan[ahead][2] is None or plan[ahead][2] < i - 2 or ahead == i):
            fetch, _, before = plan[ahead]
            if before is not None:
                plan[before][1]().wait()
                done.add(before)
            fetch().start()
            ahead += 1
        plan[i][0]().wait()
        plan[i][1]().start()
    for i in range(len(plan)):
        if i not in done:
            plan[i][1]().wait()


def chunks(side, layers, shapes, late, wanted):
    for which, shape in sorted(enumerate(shapes), key=lambda one: one[0] in late):
        for layer in range(layers):
            turn = late.index(which) * layers + layer if which in late else None
            for c in range(2):
                for h in range(2):
                    for by in range(side):
                        arrives = (by == 2) and turn is not None
                        if arrives == wanted:
                            yield which, layer, turn, c, h, by


def settle(side, layers, shapes, late, *refs):
    n = len(shapes)
    temps, news = refs[: 3 * n], refs[3 * n + 4 : 6 * n + 4]
    passed = refs[3 * n : 3 * n + 4]
    *slots, inward, outward = refs[6 * n + 4 :]
    kinds = list(dict.fromkeys(shapes))
    me = lax.axis_index("dp")
    xy = (lax.div(me, side), lax.rem(me, side))
    moves = []
    for i in range(n, 3 * n):
        for layer in range(layers):
            moves.append((temps[i].at[layer], news[i].at[layer], ("f", shapes[i % n])))
    for which, layer, turn, c, h, by in chunks(side, layers, shapes, late, False):
        quarter = halves(shapes[which])[1](2 * c + h)
        i = lax.rem(xy[c] + by, side)
        there = (layer, i, slice(None), *quarter) if c == 0 else (layer, slice(None), i, *quarter)
        behind = side - 1 if h == 0 else 1
        src = passed[2 * c + h].at[turn] if turn is not None and by == behind else temps[which].at[there]
        moves.append((src, news[which].at[there], ("b", shapes[which])))
    move(moves, dict(zip([(a, k) for k in kinds for a in "bf"], slots, strict=True)), (inward, outward))


def place(side, layers, shapes, late, *refs):
    n = len(late)
    came, news = refs[n : n + 4], refs[n + 4 : 2 * n + 4]
    slots, inward, outward = refs[2 * n + 4 :]
    me = lax.axis_index("dp")
    xy = (lax.div(me, side), lax.rem(me, side))
    moves = []
    for which, layer, turn, c, h, by in chunks(side, layers, shapes, late, True):
        quarter = halves(shapes[which])[1](2 * c + h)
        i = lax.rem(xy[c] + by, side)
        there = (layer, i, slice(None), *quarter) if c == 0 else (layer, slice(None), i, *quarter)
        moves.append((came[2 * c + h].at[turn], news[late.index(which)].at[there], "b"))
    move(moves, {"b": slots}, (inward, outward))


def solution(mesh):
    side = math.isqrt(mesh.shape["dp"])

    def step(*arrays):
        terms, weights, m, v = (arrays[i : i + 3] for i in (0, 3, 6, 9))
        shapes = tuple(one.shape[1:] for one in m)
        layers = m[0].shape[0]
        late = tuple(i for i, shape in enumerate(shapes) if shape == shapes[0])
        split = [(layers, side, side, *shape) for shape in shapes]
        temps, passed = step_kernel(
            side,
            layers,
            shapes,
            late,
            [t[0].reshape(s) for t, s in zip(terms, split, strict=True)],
            [w.reshape(s) for w, s in zip(weights, split, strict=True)],
            m,
            v,
        )
        came = []
        for c in range(2):
            for by in (1, -1):
                ring = []
                for i in range(side):
                    for j in range(side):
                        to = ((i + by) % side, j) if c == 0 else (i, (j + by) % side)
                        ring.append((i * side + j, to[0] * side + to[1]))
                came.append(lax.ppermute(passed[len(came)], "dp", ring))
        anywhere = pl.BlockSpec(memory_space=pl.ANY)
        kinds = list(dict.fromkeys(shapes))
        slots = []
        for shape in kinds:
            slots += [pltpu.VMEM((SLOTS, side, *halves(shape)[0]), jnp.bfloat16), pltpu.VMEM((SLOTS_F, *shape), jnp.float32)]
        count = len(list(chunks(side, layers, shapes, late, False))) + 2 * len(shapes) * layers
        bytes_moved = 2 * sum(one.size * one.dtype.itemsize for one in temps)
        new = list(pl.pallas_call(
            functools.partial(settle, side, layers, shapes, late),
            out_shape=[jax.ShapeDtypeStruct(one.shape, one.dtype) for one in temps],
            in_specs=[anywhere] * (len(temps) + 4),
            out_specs=[anywhere] * len(temps),
            scratch_shapes=[*slots, pltpu.SemaphoreType.DMA((count,)), pltpu.SemaphoreType.DMA((count,))],
            compiler_params=pltpu.CompilerParams(vmem_limit_bytes=67_043_328),
            cost_estimate=pl.CostEstimate(flops=10**9, bytes_accessed=bytes_moved, transcendentals=0),
            name="settle",
        )(*temps, *passed))
        arriving = len(list(chunks(side, layers, shapes, late, True)))
        last = pl.pallas_call(
            functools.partial(place, side, layers, shapes, late),
            out_shape=[jax.ShapeDtypeStruct(new[i].shape, new[i].dtype) for i in late],
            in_specs=[anywhere] * (len(late) + 4),
            out_specs=[anywhere] * len(late),
            scratch_shapes=[
                pltpu.VMEM((arriving, side, *halves(shapes[0])[0]), jnp.bfloat16),
                pltpu.SemaphoreType.DMA((arriving,)),
                pltpu.SemaphoreType.DMA((arriving,)),
            ],
            input_output_aliases={i: i for i in range(len(late))},
            compiler_params=pltpu.CompilerParams(vmem_limit_bytes=67_043_328),
            name="place",
        )(*[new[i] for i in late], *came)
        for i, one in zip(late, last, strict=True):
            new[i] = one
        return (*(one.reshape(w.shape) for one, w in zip(new[:3], weights, strict=True)), *new[3:])

    all_of, cut = P(None, None, None), P(None, "dp", None)
    return jax.shard_map(
        step,
        mesh=mesh,
        in_specs=(P(("rep", "dp"), None, None, None),) * 3 + (all_of,) * 3 + (cut,) * 6,
        out_specs=(P("rep", None, None),) * 3 + (P("rep", "dp", None),) * 6,
        check_vma=False,
    )
```

```python
import functools
import math

import jax
import jax.numpy as jnp
from jax import lax
from jax.experimental import pallas as pl
from jax.experimental.pallas import tpu as pltpu
from jax.sharding import PartitionSpec as P

MESH = pl.DeviceIdType.MESH
S1, S2A, S2B, T1, T2A, T2B, A1, A1F, A2, A2F = range(10)
ARRIVALS = (0, 1, 1, 2, 3, 3, 4, 5, 6, 7)
DEPARTURES = (0, 1, 1, 0, 0, 0, 2, 0, 3, 4)
TURNS = 3
STAGES = 9


def halves(shape):
    rows, columns = shape
    if rows % 32 == 0:
        return (rows // 4, columns), lambda i, n=1: (pl.ds(i * (rows // 4), n * (rows // 4)), slice(None))
    return (rows, columns // 4), lambda i, n=1: (slice(None), pl.ds(i * (columns // 4), n * (columns // 4)))


def pieces(shape):
    rows, columns = shape
    if rows <= 64:
        n = next(k for k in (5, 3, 2, 1) if columns % (k * 128) == 0)
        return n, lambda i: (slice(None), pl.ds(pl.multiple_of(i * (columns // n), 128), columns // n))
    n = next(k for k in (5, 4, 2, 1) if rows % (k * 8) == 0)
    return n, lambda i: (pl.ds(pl.multiple_of(i * (rows // n), 8), rows // n), slice(None))


def ordered(layers, shapes):
    main = [(i, layer) for i, shape in enumerate(shapes) if shape == shapes[0] for layer in range(layers)]
    rest = [(i, layer) for i, shape in enumerate(shapes) if shape != shapes[0] for layer in range(layers)]
    return rest[:-1] + main + rest[-1:], len(rest) - 1


def kernel(side, layers, shapes, *refs):
    n = len(shapes)
    gs, ws, ms, vs, outs, mouts, vouts = (refs[i * n : (i + 1) * n] for i in range(7))
    passed = refs[7 * n : 7 * n + 8]
    scratch = refs[7 * n + 8 : -4]
    send, recv, local, stored = refs[-4:]
    kinds = list(dict.fromkeys(shapes))
    per = len(scratch) // len(kinds)
    held = {shape: scratch[i * per : (i + 1) * per] for i, shape in enumerate(kinds)}
    jobs, seen = [], {shape: 0 for shape in kinds}
    order, first_late = ordered(layers, shapes)
    for which, layer in order:
        jobs.append((which, layer, shapes[which], seen[shapes[which]]))
        seen[shapes[which]] += 1

    me = lax.axis_index("dp")
    xy = (lax.div(me, side), lax.rem(me, side))

    def at(i, by):
        return lax.rem(i + (by + side), side)

    def place(c):
        return xy[c], xy[1 - c]

    def pair(c, p, s):
        return (p, s) if c == 0 else (s, p)

    def device(c, p, s):
        a, b = pair(c, p, s)
        return {"dp": a * side + b}

    signs = (1, -1)
    barrier = pltpu.get_barrier_semaphore()
    for c in range(2):
        p, s = place(c)
        for by in signs:
            pl.semaphore_signal(barrier, inc=1, device_id=device(c, at(p, by), s), device_id_type=MESH)
    pl.semaphore_wait(barrier, 4)

    def handed(q, c, d):
        return passed[4 + 2 * c + d] if q == len(jobs) - 1 else passed[2 * c + d].at[q - first_late]

    def copy(q, c, d, kind):
        which, layer, shape, slot = jobs[q]
        r1, r2, q1, q2, oc, ob, mb, vb, wb, wn = held[shape]
        quarter, index = halves(shape)
        g, out = gs[which], outs[which]
        p, s = place(c)
        by = signs[d]

        def chunk(i, h):
            return g.at[(layer, i, slice(None), *index(2 * c + h))] if c == 0 else g.at[(layer, slice(None), i, *index(2 * c + h))]

        def block(i, j, h=0, width=2):
            return out.at[(layer, *pair(c, i, j), *index(2 * c + h, width))]

        def row(i, h=0, width=2):
            return block(i, slice(None), h, width)

        along = device(c, at(p, by), s)
        across = device(c, p, at(s, by))
        if kind == S1:
            src, dst, to = chunk(at(p, 2), d), r1.at[slot, c, d], along
        elif kind == S2A:
            src, dst, to = chunk(at(p, by), 1 - d), r2.at[slot, c, d, 1 - d], along
        elif kind == S2B:
            src, dst, to = r1.at[slot, c, d], r2.at[slot, c, d, d], along
        elif kind == T1:
            src, dst, to = oc.at[slot, c, d, at(s, 2)], q1.at[slot, c, d], across
        elif kind == T2A:
            src, dst, to = oc.at[slot, c, 1 - d, at(s, by)], q2.at[slot, c, d, 1 - d], across
        elif kind == T2B:
            src, dst, to = q1.at[slot, c, d], q2.at[slot, c, d, d], across
        elif kind == A1:
            src, dst, to = wn.at[slot, c], block(p, s), across
        elif kind == A1F:
            src, dst, to = block(p, at(s, -by), d, 1), block(p, at(s, -by), d, 1), across
        elif kind == A2 and q >= first_late:
            src, dst, to = row(p, 1 - d, 1), row(p, 1 - d, 1), along
        elif q >= first_late:
            src, dst, to = row(p, d, 1), handed(q, c, d), along
        elif kind == A2:
            src, dst, to = row(p), row(p), along
        else:
            src, dst, to = row(at(p, -by), d, 1), row(at(p, -by), d, 1), along
        return pltpu.make_async_remote_copy(
            src_ref=src,
            dst_ref=dst,
            send_sem=send.at[q, DEPARTURES[A2 if q >= first_late and kind == A2F else kind]],
            recv_sem=recv.at[q, ARRIVALS[A2 if q >= first_late and kind == A2F else kind]],
            device_id=to,
            device_id_type=MESH,
        )

    each = [(c, d) for c in range(2) for d in range(2)]

    def start(q, kind):
        for c, d in each:
            copy(q, c, d, kind).start()

    def amount(q, quarters):
        which, layer, shape, slot = jobs[q]
        out = outs[which]
        if quarters >= 4:
            return out.at[layer, pl.ds(0, quarters // 4)]
        return out.at[layer, 0, pl.ds(0, quarters * side // 4)]

    def taken(sem, ref):
        pltpu.make_async_copy(ref, ref, sem).wait()

    def arrived(q, kind):
        quarters = {S1: 4, S2A: 8, T1: 1, T2A: 2, A1: 2, A1F: 1, A2: 8, A2F: 4}[kind]
        taken(recv.at[q, ARRIVALS[kind]], amount(q, quarters))

    def own(q, c, d, kept):
        which, layer, shape, slot = jobs[q]
        oc, ob = held[shape][4:6]
        _, index = halves(shape)
        p, _ = place(c)
        g = gs[which]

        def chunk(i, h):
            return g.at[(layer, i, slice(None), *index(2 * c + h))] if c == 0 else g.at[(layer, slice(None), i, *index(2 * c + h))]

        if kept:
            return pltpu.make_async_copy(chunk(p, d), oc.at[slot, c, d], local.at[q % TURNS, 1])
        return pltpu.make_async_copy(chunk(at(p, signs[d]), d), ob.at[slot % 2, c, d], local.at[q % TURNS, 0])

    def state(q):
        which, layer, shape, slot = jobs[q]
        mb, vb, wb = held[shape][6:9]
        sources = (ms[which].at[layer], vs[which].at[layer], ws[which].at[layer, xy[0], xy[1]])
        return [
            pltpu.make_async_copy(src, buffer.at[slot % 2], local.at[q % TURNS, 2 + i])
            for i, (src, buffer) in enumerate(zip(sources, (mb, vb, wb), strict=True))
        ]

    def weight(q, c):
        which, layer, shape, slot = jobs[q]
        mine = outs[which].at[(layer, xy[0], xy[1], *halves(shape)[1](2 * c, 2))]
        return pltpu.make_async_copy(held[shape][9].at[slot, c], mine, local.at[q % TURNS, 5])

    def moments(q):
        which, layer, shape, slot = jobs[q]
        return [
            pltpu.make_async_copy(buffer.at[slot % 2], out[which].at[layer], stored.at[q, i])
            for i, (buffer, out) in enumerate(zip(held[shape][6:8], (mouts, vouts), strict=True))
        ]

    def walk(shape, body):
        steps, piece = pieces(halves(shape)[0])

        @pl.loop(0, steps)
        def _(i):
            body(piece(i))

    def add(shape, *todo):
        def body(where):
            for (ref, lead), terms in todo:
                parts = [t[(*at_, *where)].astype(jnp.float32) for t, at_ in terms]
                ref[(*lead, *where)] = functools.reduce(lambda a, b: a + b, parts).astype(ref.dtype)

        walk(shape, body)

    def stage(k, q):
        which, layer, shape, slot = jobs[q]
        r1, r2, q1, q2, oc, ob, mb, vb, wb, wn = held[shape]
        _, index = halves(shape)
        if k == 0:
            start(q, S1)
            start(q, S2A)
            for c, d in each:
                own(q, c, d, False).start()
                own(q, c, d, True).start()
        elif k == 1:
            arrived(q, S1)
            taken(local.at[q % TURNS, 0], ob.at[slot % 2])
            for c, d in each:

                @pl.loop(0, side)
                def _(j, c=c, d=d):
                    there = (slot, c, d, j)
                    add(shape, ((r1, there), ((r1, there), (ob, (slot % 2, c, d, j)))))

                copy(q, c, d, S2B).start()
        elif k == 2:
            arrived(q, S2A)
            taken(local.at[q % TURNS, 1], oc.at[slot])
            for c in range(2):
                s = place(c)[1]
                for h, j in ((0, at(s, 2)), (1, at(s, 2)), (1, at(s, 1)), (0, at(s, -1))):
                    here = (slot, c, h, j)
                    add(shape, ((oc, here), ((oc, here), (r2, (slot, c, 0, h, j)), (r2, (slot, c, 1, h, j)))))
            start(q, T1)
            start(q, T2A)
        elif k == 3:
            if slot >= 2:
                for one in moments(next(i for i, job in enumerate(jobs) if job[2:] == (shape, slot - 2))):
                    one.wait()
            for one in state(q):
                one.start()
            arrived(q, T1)
            for c, d in each:
                s = place(c)[1]
                j = at(s, signs[d])
                here = (slot, c, d)
                add(shape, ((q1, here), ((oc, (*here, j)), (r2, (slot, c, 0, d, j)), (r2, (slot, c, 1, d, j)), (q1, here))))
                copy(q, c, d, T2B).start()
        elif k == 4:
            arrived(q, T2A)
            for one in state(q):
                one.wait()
            for c in range(2):
                s = place(c)[1]
                for h in range(2):
                    terms = [(oc, (slot, c, h, s))] + [(r2, (slot, c, d, h, s)) for d in range(2)] + [(q2, (slot, c, d, h)) for d in range(2)]
                    quarter = index(2 * c + h)
                    offsets = [x.start if isinstance(x, pl.Slice) else 0 for x in quarter]
                    half = [x.start if isinstance(x, pl.Slice) else 0 for x in index(h)]

                    def body(where, c=c, h=h, terms=terms, offsets=offsets, half=half):
                        def shifted(by):
                            full = []
                            for w, size, o in zip(where, halves(shape)[0], by, strict=True):
                                full.append(pl.ds(o, size) if isinstance(w, slice) else pl.ds(o + w.start, w.size))
                            return tuple(full)

                        g = functools.reduce(lambda a, b: a + b, [t[(*lead, *where)].astype(jnp.float32) for t, lead in terms])
                        g = g.astype(jnp.bfloat16).astype(jnp.float32)
                        there = (slot % 2, *shifted(offsets))
                        w = wb[there].astype(jnp.float32)
                        m = 0.9 * mb[there] + 0.1 * g
                        v = 0.95 * vb[there] + 0.05 * g * g
                        mb[there] = m
                        vb[there] = v
                        new = w - 0.02 * (m * lax.rsqrt(v + 1e-8) + 0.1 * w)
                        wn[(slot, c, *shifted(half))] = new.astype(jnp.bfloat16)

                    walk(shape, body)
                for d in range(2):
                    copy(q, c, d, A1).start()
                weight(q, c).start()
            for one in moments(q):
                one.start()
        elif k == 5:
            arrived(q, A1)
            start(q, A1F)
        elif k == 6:
            taken(local.at[q % TURNS, 5], wn.at[slot])
            arrived(q, A1F)
            if q >= first_late:
                start(q, A2F)
            start(q, A2)
        elif k == 7:
            arrived(q, A2)
            if q < first_late:
                start(q, A2F)
        elif q < first_late:
            arrived(q, A2F)

    for t in range(len(jobs) + STAGES - 1):
        for k in range(STAGES):
            if 0 <= t - k < len(jobs):
                stage(k, t - k)

    for q, (_, _, shape, slot) in enumerate(jobs):
        if slot + 2 >= seen[shape]:
            for one in moments(q):
                one.wait()
        for i, quarters in enumerate((8, 8, 2, 8, 4) if q < first_late else (8, 8, 2, 8)):
            taken(send.at[q, i], amount(q, quarters))


def step_kernel(side, layers, shapes, terms, weights, m, v):
    scratch = []
    for shape in dict.fromkeys(shapes):
        count = layers * shapes.count(shape)
        quarter, _ = halves(shape)
        both = (quarter[0] * 2, quarter[1]) if quarter[1] == shape[1] else (quarter[0], quarter[1] * 2)
        scratch += [
            pltpu.VMEM((count, 2, 2, side, *quarter), jnp.bfloat16),
            pltpu.VMEM((count, 2, 2, 2, side, *quarter), jnp.bfloat16),
            pltpu.VMEM((count, 2, 2, *quarter), jnp.bfloat16),
            pltpu.VMEM((count, 2, 2, 2, *quarter), jnp.bfloat16),
            pltpu.VMEM((count, 2, 2, side, *quarter), jnp.bfloat16),
            pltpu.VMEM((2, 2, 2, side, *quarter), jnp.bfloat16),
            pltpu.VMEM((2, *shape), jnp.float32),
            pltpu.VMEM((2, *shape), jnp.float32),
            pltpu.VMEM((2, *shape), jnp.bfloat16),
            pltpu.VMEM((count, 2, *both), jnp.bfloat16),
        ]
    jobs = layers * len(shapes)
    order, first_late = ordered(layers, shapes)
    passed = [(jobs - 1 - first_late, side, *halves(shapes[0])[0])] * 4 + [(side, *halves(shapes[order[-1][0]])[0])] * 4
    anywhere = pl.BlockSpec(memory_space=pl.ANY)
    outs = pl.pallas_call(
        functools.partial(kernel, side, layers, shapes),
        out_shape=[jax.ShapeDtypeStruct(w.shape, jnp.bfloat16) for w in weights]
        + [jax.ShapeDtypeStruct(one.shape, jnp.float32) for one in (*m, *v)]
        + [jax.ShapeDtypeStruct(one, jnp.bfloat16) for one in passed],
        in_specs=[anywhere] * (4 * len(shapes)),
        out_specs=[anywhere] * (3 * len(shapes) + 8),
        scratch_shapes=scratch
        + [
            pltpu.SemaphoreType.DMA((jobs, 5)),
            pltpu.SemaphoreType.DMA((jobs, 8)),
            pltpu.SemaphoreType.DMA((TURNS, 6)),
            pltpu.SemaphoreType.DMA((jobs, 2)),
        ],
        compiler_params=pltpu.CompilerParams(collective_id=0, has_side_effects=True, vmem_limit_bytes=67_043_328),
        name="step",
    )(*terms, *weights, *m, *v)
    return outs[:-8], outs[-8:]


def move(moves, slots):
    plan, turns = [], {}
    for src, dst, name in moves:
        buffer, inward, outward = slots[name]
        turn = turns.setdefault(name, [])
        n = len(turn)
        at = n % buffer.shape[0]
        before = turn[n - buffer.shape[0]] if n >= buffer.shape[0] else None
        turn.append(len(plan))
        into = functools.partial(pltpu.make_async_copy, src, buffer.at[at], inward.at[at])
        out_of = functools.partial(pltpu.make_async_copy, buffer.at[at], dst, outward.at[at])
        plan.append((into, out_of, before))
    done = set()
    ahead = 0
    for i in range(len(plan)):
        while ahead < len(plan) and (plan[ahead][2] is None or plan[ahead][2] < i - 2 or ahead == i):
            fetch, _, before = plan[ahead]
            if before is not None:
                plan[before][1]().wait()
                done.add(before)
            fetch().start()
            ahead += 1
        plan[i][0]().wait()
        plan[i][1]().start()
    for i in range(len(plan)):
        if i not in done:
            plan[i][1]().wait()


def chunk(ref, layer, c, h, i, shape):
    quarter = halves(shape)[1](2 * c + h)
    return ref.at[(layer, i, slice(None), *quarter)] if c == 0 else ref.at[(layer, slice(None), i, *quarter)]


def position(side):
    me = lax.axis_index("dp")
    return lax.div(me, side), lax.rem(me, side)


def settle(side, layers, shapes, *refs):
    n = len(shapes)
    temps, news = refs[: 3 * n], refs[3 * n + 8 : 6 * n + 8]
    passed = refs[3 * n : 3 * n + 8]
    slots = refs[6 * n + 8 :]
    kinds = list(dict.fromkeys(shapes))
    names = {(a, k): slots[9 * i + 3 * j : 9 * i + 3 * j + 3] for i, k in enumerate(kinds) for j, a in enumerate(("moment", "part", "row"))}
    xy = position(side)
    moves = []
    for i in range(n, 3 * n):
        for layer in range(layers):
            moves.append((temps[i].at[layer], news[i].at[layer], ("moment", shapes[i % n])))
    order, first_late = ordered(layers, shapes)
    for q, (which, layer) in enumerate(order):
        temp, new, shape = temps[which], news[which], shapes[which]
        if q < first_late:
            for i in range(side):
                moves.append((temp.at[layer, i], new.at[layer, i], ("row", shape)))
            continue
        for c in range(2):
            for h in range(2):
                for by in (0, 1, side - 1):
                    there = (layer, c, h, lax.rem(xy[c] + by, side), shape)
                    src = chunk(temp, *there)
                    if by == (side - 1, 1)[h]:
                        src = passed[4 + 2 * c + h] if q == len(order) - 1 else passed[2 * c + h].at[q - first_late]
                    moves.append((src, chunk(new, *there), ("part", shape)))
    move(moves, names)


def place(side, layers, shapes, jobs, weights, *refs):
    n = len(weights)
    came, news = refs[n : n + 4], refs[n + 5 : 2 * n + 5]
    xy = position(side)
    moves = []
    for turn, (which, layer) in enumerate(jobs):
        for c in range(2):
            for h in range(2):
                src = came[2 * c + h].at[turn] if len(jobs) > 1 else came[2 * c + h]
                there = (layer, c, h, lax.rem(xy[c] + 2, side), shapes[which])
                moves.append((src, chunk(news[weights.index(which)], *there), "part"))
    move(moves, {"part": refs[2 * n + 5 :]})


def solution(mesh):
    side = math.isqrt(mesh.shape["dp"])

    def step(*arrays):
        terms, weights, m, v = (arrays[i : i + 3] for i in (0, 3, 6, 9))
        shapes = tuple(one.shape[1:] for one in m)
        layers = m[0].shape[0]
        split = [(layers, side, side, *shape) for shape in shapes]
        temps, passed = step_kernel(
            side,
            layers,
            shapes,
            [t[0].reshape(s) for t, s in zip(terms, split, strict=True)],
            [w.reshape(s) for w, s in zip(weights, split, strict=True)],
            m,
            v,
        )
        rings = []
        for c in range(2):
            for by in (1, -1):
                ring = []
                for i in range(side):
                    for j in range(side):
                        to = ((i + by) % side, j) if c == 0 else (i, (j + by) % side)
                        ring.append((i * side + j, to[0] * side + to[1]))
                rings.append(ring)
        came = [lax.ppermute(one, "dp", rings[i % 4]) for i, one in enumerate(passed)]
        anywhere = pl.BlockSpec(memory_space=pl.ANY)

        def slots(count, shape, dtype):
            return [pltpu.VMEM((count, *shape), dtype), pltpu.SemaphoreType.DMA((count,)), pltpu.SemaphoreType.DMA((count,))]

        room = []
        for shape in dict.fromkeys(shapes):
            room += slots(8, shape, jnp.float32) + slots(16, (side, *halves(shape)[0]), jnp.bfloat16)
            room += slots(4 if shape != shapes[0] else 1, (side, *shape), jnp.bfloat16)
        bytes_moved = 2 * sum(one.size * one.dtype.itemsize for one in temps)
        new = list(pl.pallas_call(
            functools.partial(settle, side, layers, shapes),
            out_shape=[jax.ShapeDtypeStruct(one.shape, one.dtype) for one in temps],
            in_specs=[anywhere] * (len(temps) + 8),
            out_specs=[anywhere] * len(temps),
            scratch_shapes=room,
            compiler_params=pltpu.CompilerParams(vmem_limit_bytes=67_043_328),
            cost_estimate=pl.CostEstimate(flops=10**9, bytes_accessed=bytes_moved, transcendentals=0),
            name="settle",
        )(*temps, *passed))
        order, first_late = ordered(layers, shapes)
        for name, jobs, parts in (("place", order[first_late:-1], came[:4]), ("place_last", order[-1:], came[4:])):
            to = list(dict.fromkeys(which for which, _ in jobs))
            last = pl.pallas_call(
                functools.partial(place, side, layers, shapes, jobs, to),
                out_shape=[jax.ShapeDtypeStruct(new[i].shape, new[i].dtype) for i in to],
                in_specs=[anywhere] * (len(to) + 5),
                out_specs=[anywhere] * len(to),
                scratch_shapes=slots(4 * len(jobs), (side, *halves(shapes[to[0]])[0]), jnp.bfloat16),
                input_output_aliases={i: i for i in range(len(to))},
                compiler_params=pltpu.CompilerParams(vmem_limit_bytes=67_043_328),
                cost_estimate=pl.CostEstimate(flops=10**8, bytes_accessed=10**6, transcendentals=0),
                name=name,
            )(*[new[i] for i in to], *parts, new[-1] if name == "place" else new[order[first_late][0]])
            for i, one in zip(to, last, strict=True):
                new[i] = one
        return (*(one.reshape(w.shape) for one, w in zip(new[:3], weights, strict=True)), *new[3:])

    all_of, cut = P(None, None, None), P(None, "dp", None)
    return jax.shard_map(
        step,
        mesh=mesh,
        in_specs=(P(("rep", "dp"), None, None, None),) * 3 + (all_of,) * 3 + (cut,) * 6,
        out_specs=(P("rep", None, None),) * 3 + (P("rep", "dp", None),) * 6,
        check_vma=False,
    )
```

```python
import functools
import math

import jax
import jax.numpy as jnp
from jax import lax
from jax.experimental import pallas as pl
from jax.experimental.pallas import tpu as pltpu
from jax.sharding import PartitionSpec as P

MESH = pl.DeviceIdType.MESH
S1, S2A, S2B, T1, T2A, T2B, A1, A1F, A2, A2F = range(10)
ARRIVALS = (0, 1, 1, 2, 3, 3, 4, 5, 6, 7)
DEPARTURES = (0, 1, 1, 0, 0, 0, 2, 0, 3, 4)
TURNS = 3
SECOND = 2
LATER = 6000
SETTLE_VMEM, PLACE_VMEM = 56000000, 4_000_000
STAGES = 9


def halves(shape):
    rows, columns = shape
    if rows % 32 == 0:
        return (rows // 4, columns), lambda i, n=1: (pl.ds(i * (rows // 4), n * (rows // 4)), slice(None))
    return (rows, columns // 4), lambda i, n=1: (slice(None), pl.ds(i * (columns // 4), n * (columns // 4)))


def pieces(shape):
    rows, columns = shape
    if rows <= 64:
        n = next(k for k in (5, 3, 2, 1) if columns % (k * 128) == 0)
        return n, lambda i: (slice(None), pl.ds(pl.multiple_of(i * (columns // n), 128), columns // n))
    n = next(k for k in (5, 4, 2, 1) if rows % (k * 8) == 0)
    return n, lambda i: (pl.ds(pl.multiple_of(i * (rows // n), 8), rows // n), slice(None))


def ordered(layers, shapes):
    main = [(i, layer) for i, shape in enumerate(shapes) if shape == shapes[0] for layer in range(layers)]
    rest = [(i, layer) for i, shape in enumerate(shapes) if shape != shapes[0] for layer in range(layers)]
    early = max(len(rest) - SECOND, 0)
    return rest[:early] + main + rest[early:], early, early + len(main)


def kernel(side, layers, shapes, *refs):
    n = len(shapes)
    gs, ws, ms, vs, outs, mouts, vouts = (refs[i * n : (i + 1) * n] for i in range(7))
    passed = refs[7 * n : 7 * n + 8]
    scratch = refs[7 * n + 8 : -4]
    send, recv, local, stored = refs[-4:]
    kinds = list(dict.fromkeys(shapes))
    per = len(scratch) // len(kinds)
    held = {shape: scratch[i * per : (i + 1) * per] for i, shape in enumerate(kinds)}
    jobs, seen = [], {shape: 0 for shape in kinds}
    order, first_late, second = ordered(layers, shapes)
    for which, layer in order:
        jobs.append((which, layer, shapes[which], seen[shapes[which]]))
        seen[shapes[which]] += 1

    me = lax.axis_index("dp")
    xy = (lax.div(me, side), lax.rem(me, side))

    def at(i, by):
        return lax.rem(i + (by + side), side)

    def place(c):
        return xy[c], xy[1 - c]

    def pair(c, p, s):
        return (p, s) if c == 0 else (s, p)

    def device(c, p, s):
        a, b = pair(c, p, s)
        return {"dp": a * side + b}

    signs = (1, -1)
    barrier = pltpu.get_barrier_semaphore()
    for c in range(2):
        p, s = place(c)
        for by in signs:
            pl.semaphore_signal(barrier, inc=1, device_id=device(c, at(p, by), s), device_id_type=MESH)
    pl.semaphore_wait(barrier, 4)

    @pl.when(lax.rem(lax.axis_index("rep"), 2) == 0)
    def _():
        pl.delay(LATER)


    def handed(q, c, d):
        return passed[4 + 2 * c + d].at[q - second] if q >= second else passed[2 * c + d].at[q - first_late]

    def copy(q, c, d, kind):
        which, layer, shape, slot = jobs[q]
        r1, r2, q1, q2, oc, ob, mb, vb, wb, wn = held[shape]
        quarter, index = halves(shape)
        g, out = gs[which], outs[which]
        p, s = place(c)
        by = signs[d]

        def chunk(i, h):
            return g.at[(layer, i, slice(None), *index(2 * c + h))] if c == 0 else g.at[(layer, slice(None), i, *index(2 * c + h))]

        def block(i, j, h=0, width=2):
            return out.at[(layer, *pair(c, i, j), *index(2 * c + h, width))]

        def row(i, h=0, width=2):
            return block(i, slice(None), h, width)

        along = device(c, at(p, by), s)
        across = device(c, p, at(s, by))
        if kind == S1:
            src, dst, to = chunk(at(p, 2), d), r1.at[slot, c, d], along
        elif kind == S2A:
            src, dst, to = chunk(at(p, by), 1 - d), r2.at[slot, c, d, 1 - d], along
        elif kind == S2B:
            src, dst, to = r1.at[slot, c, d], r2.at[slot, c, d, d], along
        elif kind == T1:
            src, dst, to = oc.at[slot, c, d, at(s, 2)], q1.at[slot, c, d], across
        elif kind == T2A:
            src, dst, to = oc.at[slot, c, 1 - d, at(s, by)], q2.at[slot, c, d, 1 - d], across
        elif kind == T2B:
            src, dst, to = q1.at[slot, c, d], q2.at[slot, c, d, d], across
        elif kind == A1:
            src, dst, to = wn.at[slot, c], block(p, s), across
        elif kind == A1F:
            src, dst, to = block(p, at(s, -by), d, 1), block(p, at(s, -by), d, 1), across
        elif kind == A2 and q >= first_late:
            src, dst, to = row(p, 1 - d, 1), row(p, 1 - d, 1), along
        elif q >= first_late:
            src, dst, to = row(p, d, 1), handed(q, c, d), along
        elif kind == A2:
            src, dst, to = row(p), row(p), along
        else:
            src, dst, to = row(at(p, -by), d, 1), row(at(p, -by), d, 1), along
        return pltpu.make_async_remote_copy(
            src_ref=src,
            dst_ref=dst,
            send_sem=send.at[q, DEPARTURES[A2 if q >= first_late and kind == A2F else kind]],
            recv_sem=recv.at[q, ARRIVALS[A2 if q >= first_late and kind == A2F else kind]],
            device_id=to,
            device_id_type=MESH,
        )

    each = [(c, d) for c in range(2) for d in range(2)]

    def start(q, kind):
        for c, d in each:
            copy(q, c, d, kind).start()

    def amount(q, quarters):
        which, layer, shape, slot = jobs[q]
        out = outs[which]
        if quarters >= 4:
            return out.at[layer, pl.ds(0, quarters // 4)]
        return out.at[layer, 0, pl.ds(0, quarters * side // 4)]

    def taken(sem, ref):
        pltpu.make_async_copy(ref, ref, sem).wait()

    def arrived(q, kind):
        quarters = {S1: 4, S2A: 8, T1: 1, T2A: 2, A1: 2, A1F: 1, A2: 8, A2F: 4}[kind]
        taken(recv.at[q, ARRIVALS[kind]], amount(q, quarters))

    def own(q, c, d, kept):
        which, layer, shape, slot = jobs[q]
        oc, ob = held[shape][4:6]
        _, index = halves(shape)
        p, _ = place(c)
        g = gs[which]

        def chunk(i, h):
            return g.at[(layer, i, slice(None), *index(2 * c + h))] if c == 0 else g.at[(layer, slice(None), i, *index(2 * c + h))]

        if kept:
            return pltpu.make_async_copy(chunk(p, d), oc.at[slot, c, d], local.at[q % TURNS, 1])
        return pltpu.make_async_copy(chunk(at(p, signs[d]), d), ob.at[slot % 2, c, d], local.at[q % TURNS, 0])

    def state(q):
        which, layer, shape, slot = jobs[q]
        mb, vb, wb = held[shape][6:9]
        sources = (ms[which].at[layer], vs[which].at[layer], ws[which].at[layer, xy[0], xy[1]])
        return [
            pltpu.make_async_copy(src, buffer.at[slot % 2], local.at[q % TURNS, 2 + i])
            for i, (src, buffer) in enumerate(zip(sources, (mb, vb, wb), strict=True))
        ]

    def weight(q, c):
        which, layer, shape, slot = jobs[q]
        mine = outs[which].at[(layer, xy[0], xy[1], *halves(shape)[1](2 * c, 2))]
        return pltpu.make_async_copy(held[shape][9].at[slot, c], mine, local.at[q % TURNS, 5])

    def moments(q):
        which, layer, shape, slot = jobs[q]
        return [
            pltpu.make_async_copy(buffer.at[slot % 2], out[which].at[layer], stored.at[q, i])
            for i, (buffer, out) in enumerate(zip(held[shape][6:8], (mouts, vouts), strict=True))
        ]

    def walk(shape, body):
        steps, piece = pieces(halves(shape)[0])

        @pl.loop(0, steps)
        def _(i):
            body(piece(i))

    def add(shape, *todo):
        def body(where):
            for (ref, lead), terms in todo:
                parts = [t[(*at_, *where)].astype(jnp.float32) for t, at_ in terms]
                ref[(*lead, *where)] = functools.reduce(lambda a, b: a + b, parts).astype(ref.dtype)

        walk(shape, body)

    def stage(k, q):
        which, layer, shape, slot = jobs[q]
        r1, r2, q1, q2, oc, ob, mb, vb, wb, wn = held[shape]
        _, index = halves(shape)
        if k == 0:
            start(q, S1)
            start(q, S2A)
            for c, d in each:
                own(q, c, d, False).start()
                own(q, c, d, True).start()
        elif k == 1:
            arrived(q, S1)
            taken(local.at[q % TURNS, 0], ob.at[slot % 2])
            for c, d in each:

                @pl.loop(0, side)
                def _(j, c=c, d=d):
                    there = (slot, c, d, j)
                    add(shape, ((r1, there), ((r1, there), (ob, (slot % 2, c, d, j)))))

                copy(q, c, d, S2B).start()
        elif k == 2:
            arrived(q, S2A)
            taken(local.at[q % TURNS, 1], oc.at[slot])
            for c in range(2):
                s = place(c)[1]
                for h, j in ((0, at(s, 2)), (1, at(s, 2)), (1, at(s, 1)), (0, at(s, -1))):
                    here = (slot, c, h, j)
                    add(shape, ((oc, here), ((oc, here), (r2, (slot, c, 0, h, j)), (r2, (slot, c, 1, h, j)))))
            start(q, T1)
            start(q, T2A)
        elif k == 3:
            if slot >= 2:
                for one in moments(next(i for i, job in enumerate(jobs) if job[2:] == (shape, slot - 2))):
                    one.wait()
            for one in state(q):
                one.start()
            arrived(q, T1)
            for c, d in each:
                s = place(c)[1]
                j = at(s, signs[d])
                here = (slot, c, d)
                add(shape, ((q1, here), ((oc, (*here, j)), (r2, (slot, c, 0, d, j)), (r2, (slot, c, 1, d, j)), (q1, here))))
                copy(q, c, d, T2B).start()
        elif k == 4:
            arrived(q, T2A)
            for one in state(q):
                one.wait()
            for c in range(2):
                s = place(c)[1]
                for h in range(2):
                    terms = [(oc, (slot, c, h, s))] + [(r2, (slot, c, d, h, s)) for d in range(2)] + [(q2, (slot, c, d, h)) for d in range(2)]
                    quarter = index(2 * c + h)
                    offsets = [x.start if isinstance(x, pl.Slice) else 0 for x in quarter]
                    half = [x.start if isinstance(x, pl.Slice) else 0 for x in index(h)]

                    def body(where, c=c, h=h, terms=terms, offsets=offsets, half=half):
                        def shifted(by):
                            full = []
                            for w, size, o in zip(where, halves(shape)[0], by, strict=True):
                                full.append(pl.ds(o, size) if isinstance(w, slice) else pl.ds(o + w.start, w.size))
                            return tuple(full)

                        g = functools.reduce(lambda a, b: a + b, [t[(*lead, *where)].astype(jnp.float32) for t, lead in terms])
                        g = g.astype(jnp.bfloat16).astype(jnp.float32)
                        there = (slot % 2, *shifted(offsets))
                        w = wb[there].astype(jnp.float32)
                        m = 0.9 * mb[there] + 0.1 * g
                        v = 0.95 * vb[there] + 0.05 * g * g
                        mb[there] = m
                        vb[there] = v
                        new = w - 0.02 * (m * lax.rsqrt(v + 1e-8) + 0.1 * w)
                        wn[(slot, c, *shifted(half))] = new.astype(jnp.bfloat16)

                    walk(shape, body)
                for d in range(2):
                    copy(q, c, d, A1).start()
                weight(q, c).start()
            for one in moments(q):
                one.start()
        elif k == 5:
            arrived(q, A1)
            start(q, A1F)
        elif k == 6:
            taken(local.at[q % TURNS, 5], wn.at[slot])
            arrived(q, A1F)
            if q >= first_late:
                start(q, A2F)
            start(q, A2)
        elif k == 7:
            arrived(q, A2)
            if q < first_late:
                start(q, A2F)
        elif q < first_late:
            arrived(q, A2F)

    for t in range(len(jobs) + STAGES - 1):
        for k in range(STAGES):
            if 0 <= t - k < len(jobs):
                stage(k, t - k)

    for q, (_, _, shape, slot) in enumerate(jobs):
        if slot + 2 >= seen[shape]:
            for one in moments(q):
                one.wait()
        for i, quarters in enumerate((8, 8, 2, 8, 4) if q < first_late else (8, 8, 2, 8)):
            taken(send.at[q, i], amount(q, quarters))


def step_kernel(side, layers, shapes, terms, weights, m, v):
    scratch = []
    for shape in dict.fromkeys(shapes):
        count = layers * shapes.count(shape)
        quarter, _ = halves(shape)
        both = (quarter[0] * 2, quarter[1]) if quarter[1] == shape[1] else (quarter[0], quarter[1] * 2)
        scratch += [
            pltpu.VMEM((count, 2, 2, side, *quarter), jnp.bfloat16),
            pltpu.VMEM((count, 2, 2, 2, side, *quarter), jnp.bfloat16),
            pltpu.VMEM((count, 2, 2, *quarter), jnp.bfloat16),
            pltpu.VMEM((count, 2, 2, 2, *quarter), jnp.bfloat16),
            pltpu.VMEM((count, 2, 2, side, *quarter), jnp.bfloat16),
            pltpu.VMEM((2, 2, 2, side, *quarter), jnp.bfloat16),
            pltpu.VMEM((2, *shape), jnp.float32),
            pltpu.VMEM((2, *shape), jnp.float32),
            pltpu.VMEM((2, *shape), jnp.bfloat16),
            pltpu.VMEM((count, 2, *both), jnp.bfloat16),
        ]
    jobs = layers * len(shapes)
    order, first_late, second = ordered(layers, shapes)
    passed = [(second - first_late, side, *halves(shapes[0])[0])] * 4
    passed += [(jobs - second, side, *halves(shapes[order[-1][0]])[0])] * 4
    anywhere = pl.BlockSpec(memory_space=pl.ANY)
    outs = pl.pallas_call(
        functools.partial(kernel, side, layers, shapes),
        out_shape=[jax.ShapeDtypeStruct(w.shape, jnp.bfloat16) for w in weights]
        + [jax.ShapeDtypeStruct(one.shape, jnp.float32) for one in (*m, *v)]
        + [jax.ShapeDtypeStruct(one, jnp.bfloat16) for one in passed],
        in_specs=[anywhere] * (4 * len(shapes)),
        out_specs=[anywhere] * (3 * len(shapes) + 8),
        scratch_shapes=scratch
        + [
            pltpu.SemaphoreType.DMA((jobs, 5)),
            pltpu.SemaphoreType.DMA((jobs, 8)),
            pltpu.SemaphoreType.DMA((TURNS, 6)),
            pltpu.SemaphoreType.DMA((jobs, 2)),
        ],
        compiler_params=pltpu.CompilerParams(collective_id=0, has_side_effects=True, vmem_limit_bytes=67_043_328),
        name="step",
    )(*terms, *weights, *m, *v)
    return outs[:-8], outs[-8:]


def move(moves, slots):
    plan, turns = [], {}
    for src, dst, name in moves:
        buffer, inward, outward = slots[name]
        turn = turns.setdefault(name, [])
        n = len(turn)
        at = n % buffer.shape[0]
        before = turn[n - buffer.shape[0]] if n >= buffer.shape[0] else None
        turn.append(len(plan))
        into = functools.partial(pltpu.make_async_copy, src, buffer.at[at], inward.at[at])
        out_of = functools.partial(pltpu.make_async_copy, buffer.at[at], dst, outward.at[at])
        plan.append((into, out_of, before))
    done = set()
    ahead = 0
    for i in range(len(plan)):
        while ahead < len(plan) and (plan[ahead][2] is None or plan[ahead][2] < i - 2 or ahead == i):
            fetch, _, before = plan[ahead]
            if before is not None:
                plan[before][1]().wait()
                done.add(before)
            fetch().start()
            ahead += 1
        plan[i][0]().wait()
        plan[i][1]().start()
    for i in range(len(plan)):
        if i not in done:
            plan[i][1]().wait()


def chunk(ref, layer, c, h, i, shape):
    quarter = halves(shape)[1](2 * c + h)
    return ref.at[(layer, i, slice(None), *quarter)] if c == 0 else ref.at[(layer, slice(None), i, *quarter)]


def position(side):
    me = lax.axis_index("dp")
    return lax.div(me, side), lax.rem(me, side)


def settle(side, layers, shapes, *refs):
    n = len(shapes)
    temps, news = refs[: 3 * n], refs[3 * n + 8 : 6 * n + 8]
    passed = refs[3 * n : 3 * n + 8]
    slots = refs[6 * n + 8 :]
    kinds = list(dict.fromkeys(shapes))
    names = {(a, k): slots[9 * i + 3 * j : 9 * i + 3 * j + 3] for i, k in enumerate(kinds) for j, a in enumerate(("moment", "part", "row"))}
    xy = position(side)
    moves = []
    for i in range(n, 3 * n):
        for layer in range(layers):
            moves.append((temps[i].at[layer], news[i].at[layer], ("moment", shapes[i % n])))
    order, first_late, second = ordered(layers, shapes)
    for q, (which, layer) in enumerate(order):
        temp, new, shape = temps[which], news[which], shapes[which]
        if q < first_late:
            for i in range(side):
                moves.append((temp.at[layer, i], new.at[layer, i], ("row", shape)))
            continue
        for c in range(2):
            for h in range(2):
                for by in (0, 1, side - 1):
                    there = (layer, c, h, lax.rem(xy[c] + by, side), shape)
                    src = chunk(temp, *there)
                    if by == (side - 1, 1)[h]:
                        src = passed[4 + 2 * c + h].at[q - second] if q >= second else passed[2 * c + h].at[q - first_late]
                    moves.append((src, chunk(new, *there), ("part", shape)))
    move(moves, names)


def place(side, layers, shapes, jobs, weights, ordering, *refs):
    n = len(weights)
    came, news, sem = refs[n : n + 4], refs[n + 4 + ordering : 2 * n + 4 + ordering], refs[-1]
    xy = position(side)
    copies = []
    for turn, (which, layer) in enumerate(jobs):
        for c in range(2):
            for h in range(2):
                src = came[2 * c + h].at[turn]
                there = (layer, c, h, lax.rem(xy[c] + 2, side), shapes[which])
                copies.append(pltpu.make_async_copy(src, chunk(news[weights.index(which)], *there), sem.at[len(copies)]))
    for one in copies:
        one.start()
    for one in copies:
        one.wait()


def solution(mesh):
    side = math.isqrt(mesh.shape["dp"])

    def step(*arrays):
        terms, weights, m, v = (arrays[i : i + 3] for i in (0, 3, 6, 9))
        shapes = tuple(one.shape[1:] for one in m)
        layers = m[0].shape[0]
        split = [(layers, side, side, *shape) for shape in shapes]
        temps, passed = step_kernel(
            side,
            layers,
            shapes,
            [t[0].reshape(s) for t, s in zip(terms, split, strict=True)],
            [w.reshape(s) for w, s in zip(weights, split, strict=True)],
            m,
            v,
        )
        rings = []
        for c in range(2):
            for by in (1, -1):
                ring = []
                for i in range(side):
                    for j in range(side):
                        to = ((i + by) % side, j) if c == 0 else (i, (j + by) % side)
                        ring.append((i * side + j, to[0] * side + to[1]))
                rings.append(ring)
        came = [lax.ppermute(one, "dp", rings[i % 4]) for i, one in enumerate(passed)]
        anywhere = pl.BlockSpec(memory_space=pl.ANY)

        def slots(count, shape, dtype):
            return [pltpu.VMEM((count, *shape), dtype), pltpu.SemaphoreType.DMA((count,)), pltpu.SemaphoreType.DMA((count,))]

        room = []
        for shape in dict.fromkeys(shapes):
            room += slots(8, shape, jnp.float32) + slots(16, (side, *halves(shape)[0]), jnp.bfloat16)
            room += slots(4 if shape != shapes[0] else 1, (side, *shape), jnp.bfloat16)
        bytes_moved = 2 * sum(one.size * one.dtype.itemsize for one in temps)
        new = list(pl.pallas_call(
            functools.partial(settle, side, layers, shapes),
            out_shape=[jax.ShapeDtypeStruct(one.shape, one.dtype) for one in temps],
            in_specs=[anywhere] * (len(temps) + 8),
            out_specs=[anywhere] * len(temps),
            scratch_shapes=room,
            compiler_params=pltpu.CompilerParams(vmem_limit_bytes=SETTLE_VMEM),
            cost_estimate=pl.CostEstimate(flops=10**9, bytes_accessed=bytes_moved, transcendentals=0),
            name="settle",
        )(*temps, *passed))
        order, first_late, second = ordered(layers, shapes)
        order_token = []
        for name, jobs, parts in (("place", order[first_late:second], came[:4]), ("place_last", order[second:], came[4:])):
            to = list(dict.fromkeys(which for which, _ in jobs))
            token = [] if order_token else [jax.ShapeDtypeStruct((8, 128), jnp.float32)]
            *last, order_token = pl.pallas_call(
                functools.partial(place, side, layers, shapes, jobs, to, len(order_token)),
                out_shape=[jax.ShapeDtypeStruct(new[i].shape, new[i].dtype) for i in to] + token,
                in_specs=[anywhere] * (len(to) + 4 + len(order_token)),
                out_specs=[anywhere] * (len(to) + len(token)),
                scratch_shapes=[pltpu.SemaphoreType.DMA((4 * len(jobs),))],
                input_output_aliases={i: i for i in range(len(to))},
                compiler_params=pltpu.CompilerParams(vmem_limit_bytes=PLACE_VMEM),
                cost_estimate=pl.CostEstimate(flops=10**8, bytes_accessed=10**6, transcendentals=0),
                name=name,
            )(*[new[i] for i in to], *parts, *order_token)
            last, order_token = (last, [order_token]) if token else ([*last, order_token], [])
            for i, one in zip(to, last, strict=True):
                new[i] = one
        return (*(one.reshape(w.shape) for one, w in zip(new[:3], weights, strict=True)), *new[3:])

    all_of, cut = P(None, None, None), P(None, "dp", None)
    return jax.shard_map(
        step,
        mesh=mesh,
        in_specs=(P(("rep", "dp"), None, None, None),) * 3 + (all_of,) * 3 + (cut,) * 6,
        out_specs=(P("rep", None, None),) * 3 + (P("rep", "dp", None),) * 6,
        check_vma=False,
    )
```

```python
import functools
import math

import jax
import jax.numpy as jnp
from jax import lax
from jax.experimental import pallas as pl
from jax.experimental.pallas import tpu as pltpu
from jax.sharding import PartitionSpec as P

MESH = pl.DeviceIdType.MESH
S1, S2A, S2B, T1, T2A, T2B, A1, A1F, A2, A2P = range(10)
ARRIVALS = (0, 1, 1, 2, 3, 3, 4, 5, 6, 6)
DEPARTURES = (0, 1, 1, 0, 0, 0, 2, 0, 3, 3)
TURNS = 3
LATER = 7000
SETTLE_VMEM, PLACE_VMEM = 56000000, 4_000_000
STAGES = 8


def halves(shape):
    rows, columns = shape
    if rows % 32 == 0:
        return (rows // 4, columns), lambda i, n=1: (pl.ds(i * (rows // 4), n * (rows // 4)), slice(None))
    return (rows, columns // 4), lambda i, n=1: (slice(None), pl.ds(i * (columns // 4), n * (columns // 4)))


def pieces(shape):
    rows, columns = shape
    if rows <= 64:
        n = next(k for k in (5, 3, 2, 1) if columns % (k * 128) == 0)
        return n, lambda i: (slice(None), pl.ds(pl.multiple_of(i * (columns // n), 128), columns // n))
    n = next(k for k in (5, 4, 2, 1) if rows % (k * 8) == 0)
    return n, lambda i: (pl.ds(pl.multiple_of(i * (rows // n), 8), rows // n), slice(None))


def ordered(layers, shapes):
    main = [(i, layer) for i, shape in enumerate(shapes) if shape == shapes[0] for layer in range(layers)]
    rest = [(i, layer) for i, shape in enumerate(shapes) if shape != shapes[0] for layer in range(layers)]
    return main + rest, [range(len(main)), range(len(main), len(main) + len(rest))]


def handed(arrays, groups, q, c, d):
    i = next(i for i, group in enumerate(groups) if q in group)
    return arrays[4 * i + 2 * c + d].at[q - groups[i].start]


def kernel(side, layers, shapes, *refs):
    n = len(shapes)
    gs, ws, ms, vs, outs, mouts, vouts = (refs[i * n : (i + 1) * n] for i in range(7))
    order, groups = ordered(layers, shapes)
    passed = refs[7 * n : 7 * n + 4 * len(groups)]
    scratch = refs[7 * n + 4 * len(groups) : -4]
    send, recv, local, stored = refs[-4:]
    kinds = list(dict.fromkeys(shapes))
    per = len(scratch) // len(kinds)
    held = {shape: scratch[i * per : (i + 1) * per] for i, shape in enumerate(kinds)}
    jobs, seen = [], {shape: 0 for shape in kinds}
    for which, layer in order:
        jobs.append((which, layer, shapes[which], seen[shapes[which]]))
        seen[shapes[which]] += 1

    me = lax.axis_index("dp")
    xy = (lax.div(me, side), lax.rem(me, side))

    def at(i, by):
        return lax.rem(i + (by + side), side)

    def place(c):
        return xy[c], xy[1 - c]

    def pair(c, p, s):
        return (p, s) if c == 0 else (s, p)

    def device(c, p, s):
        a, b = pair(c, p, s)
        return {"dp": a * side + b}

    signs = (1, -1)
    barrier = pltpu.get_barrier_semaphore()
    for c in range(2):
        p, s = place(c)
        for by in signs:
            pl.semaphore_signal(barrier, inc=1, device_id=device(c, at(p, by), s), device_id_type=MESH)
    pl.semaphore_wait(barrier, 4)

    @pl.when(lax.rem(lax.axis_index("rep"), 2) == 0)
    def _():
        pl.delay(LATER)


    def copy(q, c, d, kind):
        which, layer, shape, slot = jobs[q]
        r1, r2, q1, q2, oc, ob, mb, vb, wb, wn = held[shape]
        quarter, index = halves(shape)
        g, out = gs[which], outs[which]
        p, s = place(c)
        by = signs[d]

        def chunk(i, h):
            return g.at[(layer, i, slice(None), *index(2 * c + h))] if c == 0 else g.at[(layer, slice(None), i, *index(2 * c + h))]

        def block(i, j, h=0, width=2):
            return out.at[(layer, *pair(c, i, j), *index(2 * c + h, width))]

        def row(i, h=0, width=2):
            return block(i, slice(None), h, width)

        along = device(c, at(p, by), s)
        across = device(c, p, at(s, by))
        if kind == S1:
            src, dst, to = chunk(at(p, 2), d), r1.at[slot, c, d], along
        elif kind == S2A:
            src, dst, to = chunk(at(p, by), 1 - d), r2.at[slot, c, d, 1 - d], along
        elif kind == S2B:
            src, dst, to = r1.at[slot, c, d], r2.at[slot, c, d, d], along
        elif kind == T1:
            src, dst, to = oc.at[slot, c, d, at(s, 2)], q1.at[slot, c, d], across
        elif kind == T2A:
            src, dst, to = oc.at[slot, c, 1 - d, at(s, by)], q2.at[slot, c, d, 1 - d], across
        elif kind == T2B:
            src, dst, to = q1.at[slot, c, d], q2.at[slot, c, d, d], across
        elif kind == A1:
            src, dst, to = wn.at[slot, c], block(p, s), across
        elif kind == A1F:
            src, dst, to = block(p, at(s, -by), d, 1), block(p, at(s, -by), d, 1), across
        elif kind == A2:
            src, dst, to = row(p, 1 - d, 1), row(p, 1 - d, 1), along
        else:
            src, dst, to = row(p, d, 1), handed(passed, groups, q, c, d), along
        return pltpu.make_async_remote_copy(
            src_ref=src,
            dst_ref=dst,
            send_sem=send.at[q, DEPARTURES[kind]],
            recv_sem=recv.at[q, ARRIVALS[kind]],
            device_id=to,
            device_id_type=MESH,
        )

    each = [(c, d) for c in range(2) for d in range(2)]

    def start(q, kind):
        for c, d in each:
            copy(q, c, d, kind).start()

    def amount(q, quarters):
        which, layer, shape, slot = jobs[q]
        out = outs[which]
        if quarters >= 4:
            return out.at[layer, pl.ds(0, quarters // 4)]
        return out.at[layer, 0, pl.ds(0, quarters * side // 4)]

    def taken(sem, ref):
        pltpu.make_async_copy(ref, ref, sem).wait()

    def arrived(q, kind):
        quarters = {S1: 4, S2A: 8, T1: 1, T2A: 2, A1: 2, A1F: 1, A2: 8}[kind]
        taken(recv.at[q, ARRIVALS[kind]], amount(q, quarters))

    def own(q, c, d, kept):
        which, layer, shape, slot = jobs[q]
        oc, ob = held[shape][4:6]
        _, index = halves(shape)
        p, _ = place(c)
        g = gs[which]

        def chunk(i, h):
            return g.at[(layer, i, slice(None), *index(2 * c + h))] if c == 0 else g.at[(layer, slice(None), i, *index(2 * c + h))]

        if kept:
            return pltpu.make_async_copy(chunk(p, d), oc.at[slot, c, d], local.at[q % TURNS, 1])
        return pltpu.make_async_copy(chunk(at(p, signs[d]), d), ob.at[slot % 2, c, d], local.at[q % TURNS, 0])

    def state(q):
        which, layer, shape, slot = jobs[q]
        mb, vb, wb = held[shape][6:9]
        sources = (ms[which].at[layer], vs[which].at[layer], ws[which].at[layer, xy[0], xy[1]])
        return [
            pltpu.make_async_copy(src, buffer.at[slot % 2], local.at[q % TURNS, 2 + i])
            for i, (src, buffer) in enumerate(zip(sources, (mb, vb, wb), strict=True))
        ]

    def weight(q, c):
        which, layer, shape, slot = jobs[q]
        mine = outs[which].at[(layer, xy[0], xy[1], *halves(shape)[1](2 * c, 2))]
        return pltpu.make_async_copy(held[shape][9].at[slot, c], mine, local.at[q % TURNS, 5])

    def moments(q):
        which, layer, shape, slot = jobs[q]
        return [
            pltpu.make_async_copy(buffer.at[slot % 2], out[which].at[layer], stored.at[q, i])
            for i, (buffer, out) in enumerate(zip(held[shape][6:8], (mouts, vouts), strict=True))
        ]

    def walk(shape, body):
        steps, piece = pieces(halves(shape)[0])

        @pl.loop(0, steps)
        def _(i):
            body(piece(i))

    def add(shape, *todo):
        def body(where):
            for (ref, lead), terms in todo:
                parts = [t[(*at_, *where)].astype(jnp.float32) for t, at_ in terms]
                ref[(*lead, *where)] = functools.reduce(lambda a, b: a + b, parts).astype(ref.dtype)

        walk(shape, body)

    def stage(k, q):
        which, layer, shape, slot = jobs[q]
        r1, r2, q1, q2, oc, ob, mb, vb, wb, wn = held[shape]
        _, index = halves(shape)
        if k == 0:
            start(q, S1)
            start(q, S2A)
            for c, d in each:
                own(q, c, d, False).start()
                own(q, c, d, True).start()
        elif k == 1:
            arrived(q, S1)
            taken(local.at[q % TURNS, 0], ob.at[slot % 2])
            for c, d in each:

                @pl.loop(0, side)
                def _(j, c=c, d=d):
                    there = (slot, c, d, j)
                    add(shape, ((r1, there), ((r1, there), (ob, (slot % 2, c, d, j)))))

                copy(q, c, d, S2B).start()
        elif k == 2:
            arrived(q, S2A)
            taken(local.at[q % TURNS, 1], oc.at[slot])
            for c in range(2):
                s = place(c)[1]
                for h, j in ((0, at(s, 2)), (1, at(s, 2)), (1, at(s, 1)), (0, at(s, -1))):
                    here = (slot, c, h, j)
                    add(shape, ((oc, here), ((oc, here), (r2, (slot, c, 0, h, j)), (r2, (slot, c, 1, h, j)))))
            start(q, T1)
            start(q, T2A)
        elif k == 3:
            if slot >= 2:
                for one in moments(next(i for i, job in enumerate(jobs) if job[2:] == (shape, slot - 2))):
                    one.wait()
            for one in state(q):
                one.start()
            arrived(q, T1)
            for c, d in each:
                s = place(c)[1]
                j = at(s, signs[d])
                here = (slot, c, d)
                add(shape, ((q1, here), ((oc, (*here, j)), (r2, (slot, c, 0, d, j)), (r2, (slot, c, 1, d, j)), (q1, here))))
                copy(q, c, d, T2B).start()
        elif k == 4:
            arrived(q, T2A)
            for one in state(q):
                one.wait()
            for c in range(2):
                s = place(c)[1]
                for h in range(2):
                    terms = [(oc, (slot, c, h, s))] + [(r2, (slot, c, d, h, s)) for d in range(2)] + [(q2, (slot, c, d, h)) for d in range(2)]
                    quarter = index(2 * c + h)
                    offsets = [x.start if isinstance(x, pl.Slice) else 0 for x in quarter]
                    half = [x.start if isinstance(x, pl.Slice) else 0 for x in index(h)]

                    def body(where, c=c, h=h, terms=terms, offsets=offsets, half=half):
                        def shifted(by):
                            full = []
                            for w, size, o in zip(where, halves(shape)[0], by, strict=True):
                                full.append(pl.ds(o, size) if isinstance(w, slice) else pl.ds(o + w.start, w.size))
                            return tuple(full)

                        g = functools.reduce(lambda a, b: a + b, [t[(*lead, *where)].astype(jnp.float32) for t, lead in terms])
                        g = g.astype(jnp.bfloat16).astype(jnp.float32)
                        there = (slot % 2, *shifted(offsets))
                        w = wb[there].astype(jnp.float32)
                        m = 0.9 * mb[there] + 0.1 * g
                        v = 0.95 * vb[there] + 0.05 * g * g
                        mb[there] = m
                        vb[there] = v
                        new = w - 0.02 * (m * lax.rsqrt(v + 1e-8) + 0.1 * w)
                        wn[(slot, c, *shifted(half))] = new.astype(jnp.bfloat16)

                    walk(shape, body)
                for d in range(2):
                    copy(q, c, d, A1).start()
                weight(q, c).start()
            for one in moments(q):
                one.start()
        elif k == 5:
            arrived(q, A1)
            start(q, A1F)
        elif k == 6:
            taken(local.at[q % TURNS, 5], wn.at[slot])
            arrived(q, A1F)
            start(q, A2P)
            start(q, A2)
        else:
            arrived(q, A2)

    for t in range(len(jobs) + STAGES - 1):
        for k in range(STAGES):
            if 0 <= t - k < len(jobs):
                stage(k, t - k)

    for q, (_, _, shape, slot) in enumerate(jobs):
        if slot + 2 >= seen[shape]:
            for one in moments(q):
                one.wait()
        for i, quarters in enumerate((8, 8, 2, 8)):
            taken(send.at[q, i], amount(q, quarters))


def step_kernel(side, layers, shapes, terms, weights, m, v):
    scratch = []
    for shape in dict.fromkeys(shapes):
        count = layers * shapes.count(shape)
        quarter, _ = halves(shape)
        both = (quarter[0] * 2, quarter[1]) if quarter[1] == shape[1] else (quarter[0], quarter[1] * 2)
        scratch += [
            pltpu.VMEM((count, 2, 2, side, *quarter), jnp.bfloat16),
            pltpu.VMEM((count, 2, 2, 2, side, *quarter), jnp.bfloat16),
            pltpu.VMEM((count, 2, 2, *quarter), jnp.bfloat16),
            pltpu.VMEM((count, 2, 2, 2, *quarter), jnp.bfloat16),
            pltpu.VMEM((count, 2, 2, side, *quarter), jnp.bfloat16),
            pltpu.VMEM((2, 2, 2, side, *quarter), jnp.bfloat16),
            pltpu.VMEM((2, *shape), jnp.float32),
            pltpu.VMEM((2, *shape), jnp.float32),
            pltpu.VMEM((2, *shape), jnp.bfloat16),
            pltpu.VMEM((count, 2, *both), jnp.bfloat16),
        ]
    jobs = layers * len(shapes)
    order, groups = ordered(layers, shapes)
    passed = [(len(group), side, *halves(shapes[order[group[0]][0]])[0]) for group in groups for _ in range(4)]
    anywhere = pl.BlockSpec(memory_space=pl.ANY)
    outs = pl.pallas_call(
        functools.partial(kernel, side, layers, shapes),
        out_shape=[jax.ShapeDtypeStruct(w.shape, jnp.bfloat16) for w in weights]
        + [jax.ShapeDtypeStruct(one.shape, jnp.float32) for one in (*m, *v)]
        + [jax.ShapeDtypeStruct(one, jnp.bfloat16) for one in passed],
        in_specs=[anywhere] * (4 * len(shapes)),
        out_specs=[anywhere] * (3 * len(shapes) + len(passed)),
        scratch_shapes=scratch
        + [
            pltpu.SemaphoreType.DMA((jobs, 4)),
            pltpu.SemaphoreType.DMA((jobs, 7)),
            pltpu.SemaphoreType.DMA((TURNS, 6)),
            pltpu.SemaphoreType.DMA((jobs, 2)),
        ],
        compiler_params=pltpu.CompilerParams(collective_id=0, has_side_effects=True, vmem_limit_bytes=67_043_328),
        name="step",
    )(*terms, *weights, *m, *v)
    return outs[: -len(passed)], outs[-len(passed) :]


def move(moves, slots):
    plan, turns = [], {}
    for src, dst, name in moves:
        buffer, inward, outward = slots[name]
        turn = turns.setdefault(name, [])
        n = len(turn)
        at = n % buffer.shape[0]
        before = turn[n - buffer.shape[0]] if n >= buffer.shape[0] else None
        turn.append(len(plan))
        into = functools.partial(pltpu.make_async_copy, src, buffer.at[at], inward.at[at])
        out_of = functools.partial(pltpu.make_async_copy, buffer.at[at], dst, outward.at[at])
        plan.append((into, out_of, before))
    done = set()
    ahead = 0
    for i in range(len(plan)):
        while ahead < len(plan) and (plan[ahead][2] is None or plan[ahead][2] < i - 2 or ahead == i):
            fetch, _, before = plan[ahead]
            if before is not None:
                plan[before][1]().wait()
                done.add(before)
            fetch().start()
            ahead += 1
        plan[i][0]().wait()
        plan[i][1]().start()
    for i in range(len(plan)):
        if i not in done:
            plan[i][1]().wait()


def chunk(ref, layer, c, h, i, shape):
    quarter = halves(shape)[1](2 * c + h)
    return ref.at[(layer, i, slice(None), *quarter)] if c == 0 else ref.at[(layer, slice(None), i, *quarter)]


def position(side):
    me = lax.axis_index("dp")
    return lax.div(me, side), lax.rem(me, side)


def settle(side, layers, shapes, *refs):
    n = len(shapes)
    order, groups = ordered(layers, shapes)
    handing = 4 * len(groups)
    temps, passed, news = refs[: 3 * n], refs[3 * n : 3 * n + handing], refs[3 * n + handing : 6 * n + handing]
    slots = refs[6 * n + handing :]
    kinds = list(dict.fromkeys(shapes))
    names = {(a, k): slots[6 * i + 3 * j : 6 * i + 3 * j + 3] for i, k in enumerate(kinds) for j, a in enumerate(("moment", "part"))}
    xy = position(side)
    moves = []
    for i in range(n, 3 * n):
        for layer in range(layers):
            moves.append((temps[i].at[layer], news[i].at[layer], ("moment", shapes[i % n])))
    for q, (which, layer) in enumerate(order):
        for c in range(2):
            for h in range(2):
                for by in (0, 1, side - 1):
                    there = (layer, c, h, lax.rem(xy[c] + by, side), shapes[which])
                    src = handed(passed, groups, q, c, h) if by == (side - 1, 1)[h] else chunk(temps[which], *there)
                    moves.append((src, chunk(news[which], *there), ("part", shapes[which])))
    move(moves, names)


def place(side, layers, shapes, jobs, weights, ordering, *refs):
    n = len(weights)
    came, news, sem = refs[n : n + 4], refs[n + 4 + ordering : 2 * n + 4 + ordering], refs[-1]
    xy = position(side)
    copies = []
    for turn, (which, layer) in enumerate(jobs):
        for c in range(2):
            for h in range(2):
                src = came[2 * c + h].at[turn]
                there = (layer, c, h, lax.rem(xy[c] + 2, side), shapes[which])
                copies.append(pltpu.make_async_copy(src, chunk(news[weights.index(which)], *there), sem.at[len(copies)]))
    for one in copies:
        one.start()
    for one in copies:
        one.wait()


def solution(mesh):
    side = math.isqrt(mesh.shape["dp"])

    def step(*arrays):
        terms, weights, m, v = (arrays[i : i + 3] for i in (0, 3, 6, 9))
        shapes = tuple(one.shape[1:] for one in m)
        layers = m[0].shape[0]
        split = [(layers, side, side, *shape) for shape in shapes]
        temps, passed = step_kernel(
            side,
            layers,
            shapes,
            [t[0].reshape(s) for t, s in zip(terms, split, strict=True)],
            [w.reshape(s) for w, s in zip(weights, split, strict=True)],
            m,
            v,
        )
        rings = []
        for c in range(2):
            for by in (1, -1):
                ring = []
                for i in range(side):
                    for j in range(side):
                        to = ((i + by) % side, j) if c == 0 else (i, (j + by) % side)
                        ring.append((i * side + j, to[0] * side + to[1]))
                rings.append(ring)
        came = [lax.ppermute(one, "dp", rings[i % 4]) for i, one in enumerate(passed)]
        anywhere = pl.BlockSpec(memory_space=pl.ANY)

        def slots(count, shape, dtype):
            return [pltpu.VMEM((count, *shape), dtype), pltpu.SemaphoreType.DMA((count,)), pltpu.SemaphoreType.DMA((count,))]

        room = []
        for shape in dict.fromkeys(shapes):
            room += slots(8, shape, jnp.float32) + slots(16, (side, *halves(shape)[0]), jnp.bfloat16)
        bytes_moved = 2 * sum(one.size * one.dtype.itemsize for one in temps)
        new = list(pl.pallas_call(
            functools.partial(settle, side, layers, shapes),
            out_shape=[jax.ShapeDtypeStruct(one.shape, one.dtype) for one in temps],
            in_specs=[anywhere] * (len(temps) + len(passed)),
            out_specs=[anywhere] * len(temps),
            scratch_shapes=room,
            compiler_params=pltpu.CompilerParams(vmem_limit_bytes=SETTLE_VMEM),
            cost_estimate=pl.CostEstimate(flops=10**9, bytes_accessed=bytes_moved, transcendentals=0),
            name="settle",
        )(*temps, *passed))
        order, groups = ordered(layers, shapes)
        before = []
        for i, group in enumerate(groups):
            jobs = [order[q] for q in group]
            to = list(dict.fromkeys(which for which, _ in jobs))
            *last, after = pl.pallas_call(
                functools.partial(place, side, layers, shapes, jobs, to, len(before)),
                out_shape=[jax.ShapeDtypeStruct(new[w].shape, new[w].dtype) for w in to] + [jax.ShapeDtypeStruct((8, 128), jnp.float32)],
                in_specs=[anywhere] * (len(to) + 4 + len(before)),
                out_specs=[anywhere] * (len(to) + 1),
                scratch_shapes=[pltpu.SemaphoreType.DMA((4 * len(jobs),))],
                input_output_aliases={w: w for w in range(len(to))},
                compiler_params=pltpu.CompilerParams(vmem_limit_bytes=PLACE_VMEM),
                cost_estimate=pl.CostEstimate(flops=10**8, bytes_accessed=10**6, transcendentals=0),
                name=f"place_{i}",
            )(*[new[w] for w in to], *came[4 * i : 4 * i + 4], *before)
            before = [after]
            for w, one in zip(to, last, strict=True):
                new[w] = one
        return (*(one.reshape(w.shape) for one, w in zip(new[:3], weights, strict=True)), *new[3:])

    all_of, cut = P(None, None, None), P(None, "dp", None)
    return jax.shard_map(
        step,
        mesh=mesh,
        in_specs=(P(("rep", "dp"), None, None, None),) * 3 + (all_of,) * 3 + (cut,) * 6,
        out_specs=(P("rep", None, None),) * 3 + (P("rep", "dp", None),) * 6,
        check_vma=False,
    )
```

```python
import functools
import math

import jax
import jax.numpy as jnp
from jax import lax
from jax.experimental import pallas as pl
from jax.experimental.pallas import tpu as pltpu
from jax.sharding import PartitionSpec as P

MESH = pl.DeviceIdType.MESH
S1, S2A, S2B, T1, T2A, T2B, A1, A1F, A2, A2P = range(10)
ARRIVALS = (0, 1, 1, 2, 3, 3, 4, 5, 6, 6)
DEPARTURES = (0, 1, 1, 0, 0, 0, 2, 0, 3, 3)
TURNS = 3
LATER = 7000
SETTLE_VMEM, PLACE_VMEM = 56000000, 4_000_000
STAGES = 8


def halves(shape):
    rows, columns = shape
    if rows % 32 == 0:
        return (rows // 4, columns), lambda i, n=1: (pl.ds(i * (rows // 4), n * (rows // 4)), slice(None))
    return (rows, columns // 4), lambda i, n=1: (slice(None), pl.ds(i * (columns // 4), n * (columns // 4)))


def pieces(shape):
    rows, columns = shape
    if rows <= 64:
        n = next(k for k in (5, 3, 2, 1) if columns % (k * 128) == 0)
        return n, lambda i: (slice(None), pl.ds(pl.multiple_of(i * (columns // n), 128), columns // n))
    n = next(k for k in (5, 4, 2, 1) if rows % (k * 8) == 0)
    return n, lambda i: (pl.ds(pl.multiple_of(i * (rows // n), 8), rows // n), slice(None))


def ordered(layers, shapes):
    main = [(i, layer) for i, shape in enumerate(shapes) if shape == shapes[0] for layer in range(layers)]
    rest = [(i, layer) for i, shape in enumerate(shapes) if shape != shapes[0] for layer in range(layers)]
    return main + rest, [range(len(main)), range(len(main), len(main) + len(rest))]


def handed(arrays, groups, q, c, d):
    i = next(i for i, group in enumerate(groups) if q in group)
    return arrays[4 * i + 2 * c + d].at[q - groups[i].start]


def kernel(side, layers, shapes, *refs):
    n = len(shapes)
    gs, ws, ms, vs, outs, mouts, vouts = (refs[i * n : (i + 1) * n] for i in range(7))
    order, groups = ordered(layers, shapes)
    passed = refs[7 * n : 7 * n + 4 * len(groups)]
    scratch = refs[7 * n + 4 * len(groups) : -4]
    send, recv, local, stored = refs[-4:]
    kinds = list(dict.fromkeys(shapes))
    per = len(scratch) // len(kinds)
    held = {shape: scratch[i * per : (i + 1) * per] for i, shape in enumerate(kinds)}
    jobs, seen = [], {shape: 0 for shape in kinds}
    for which, layer in order:
        jobs.append((which, layer, shapes[which], seen[shapes[which]]))
        seen[shapes[which]] += 1

    me = lax.axis_index("dp")
    xy = (lax.div(me, side), lax.rem(me, side))

    def at(i, by):
        return lax.rem(i + (by + side), side)

    def place(c):
        return xy[c], xy[1 - c]

    def pair(c, p, s):
        return (p, s) if c == 0 else (s, p)

    def device(c, p, s):
        a, b = pair(c, p, s)
        return {"dp": a * side + b}

    signs = (1, -1)
    barrier = pltpu.get_barrier_semaphore()
    for c in range(2):
        p, s = place(c)
        for by in signs:
            pl.semaphore_signal(barrier, inc=1, device_id=device(c, at(p, by), s), device_id_type=MESH)
    pl.semaphore_wait(barrier, 4)

    @pl.when(lax.rem(lax.axis_index("rep"), 2) == 0)
    def _():
        pl.delay(LATER)


    def copy(q, c, d, kind):
        which, layer, shape, slot = jobs[q]
        r1, r2, q1, q2, oc, ob, mb, vb, wb, wn = held[shape]
        quarter, index = halves(shape)
        g, out = gs[which], outs[which]
        p, s = place(c)
        by = signs[d]

        def chunk(i, h):
            return g.at[(layer, i, slice(None), *index(2 * c + h))] if c == 0 else g.at[(layer, slice(None), i, *index(2 * c + h))]

        def block(i, j, h=0, width=2):
            return out.at[(layer, *pair(c, i, j), *index(2 * c + h, width))]

        def row(i, h=0, width=2):
            return block(i, slice(None), h, width)

        along = device(c, at(p, by), s)
        across = device(c, p, at(s, by))
        if kind == S1:
            src, dst, to = chunk(at(p, 2), d), r1.at[slot, c, d], along
        elif kind == S2A:
            src, dst, to = chunk(at(p, by), 1 - d), r2.at[slot, c, d, 1 - d], along
        elif kind == S2B:
            src, dst, to = r1.at[slot, c, d], r2.at[slot, c, d, d], along
        elif kind == T1:
            src, dst, to = oc.at[slot, c, d, at(s, 2)], q1.at[slot, c, d], across
        elif kind == T2A:
            src, dst, to = oc.at[slot, c, 1 - d, at(s, by)], q2.at[slot, c, d, 1 - d], across
        elif kind == T2B:
            src, dst, to = q1.at[slot, c, d], q2.at[slot, c, d, d], across
        elif kind == A1:
            src, dst, to = wn.at[slot, c], block(p, s), across
        elif kind == A1F:
            src, dst, to = block(p, at(s, -by), d, 1), block(p, at(s, -by), d, 1), across
        elif kind == A2:
            src, dst, to = row(p, 1 - d, 1), row(p, 1 - d, 1), along
        else:
            src, dst, to = row(p, d, 1), handed(passed, groups, q, c, d), along
        return pltpu.make_async_remote_copy(
            src_ref=src,
            dst_ref=dst,
            send_sem=send.at[kinds.index(shape), DEPARTURES[kind]],
            recv_sem=recv.at[q, ARRIVALS[kind]],
            device_id=to,
            device_id_type=MESH,
        )

    each = [(c, d) for c in range(2) for d in range(2)]

    def start(q, kind):
        for c, d in each:
            copy(q, c, d, kind).start()

    def amount(q, quarters):
        which, layer, shape, slot = jobs[q]
        out = outs[which]
        if quarters > 4 * side:
            return out.at[pl.ds(0, quarters // (4 * side))]
        if quarters >= 4:
            return out.at[layer, pl.ds(0, quarters // 4)]
        return out.at[layer, 0, pl.ds(0, quarters * side // 4)]

    def taken(sem, ref):
        pltpu.make_async_copy(ref, ref, sem).wait()

    def arrived(q, kind):
        quarters = {S1: 4, S2A: 8, T1: 1, T2A: 2, A1: 2, A1F: 1, A2: 8}[kind]
        taken(recv.at[q, ARRIVALS[kind]], amount(q, quarters))

    def own(q, c, d, kept):
        which, layer, shape, slot = jobs[q]
        oc, ob = held[shape][4:6]
        _, index = halves(shape)
        p, _ = place(c)
        g = gs[which]

        def chunk(i, h):
            return g.at[(layer, i, slice(None), *index(2 * c + h))] if c == 0 else g.at[(layer, slice(None), i, *index(2 * c + h))]

        if kept:
            return pltpu.make_async_copy(chunk(p, d), oc.at[slot, c, d], local.at[q % TURNS, 0])
        return pltpu.make_async_copy(chunk(at(p, signs[d]), d), ob.at[slot % 2, c, d], local.at[q % TURNS, 0])

    def state(q):
        which, layer, shape, slot = jobs[q]
        mb, vb, wb = held[shape][6:9]
        sources = (ms[which].at[layer], vs[which].at[layer], ws[which].at[layer, xy[0], xy[1]])
        return [
            pltpu.make_async_copy(src, buffer.at[slot % 2], local.at[q % TURNS, 1 + i // 2])
            for i, (src, buffer) in enumerate(zip(sources, (mb, vb, wb), strict=True))
        ]

    def weight(q, c):
        which, layer, shape, slot = jobs[q]
        mine = outs[which].at[(layer, xy[0], xy[1], *halves(shape)[1](2 * c, 2))]
        return pltpu.make_async_copy(held[shape][9].at[slot, c], mine, local.at[q % TURNS, 3])

    def moments(q):
        which, layer, shape, slot = jobs[q]
        return [
            pltpu.make_async_copy(buffer.at[slot % 2], out[which].at[layer], stored.at[kinds.index(shape), slot % 2])
            for i, (buffer, out) in enumerate(zip(held[shape][6:8], (mouts, vouts), strict=True))
        ]

    def walk(shape, body):
        steps, piece = pieces(halves(shape)[0])

        @pl.loop(0, steps)
        def _(i):
            body(piece(i))

    def add(shape, *todo):
        def body(where):
            for (ref, lead), terms in todo:
                parts = [t[(*at_, *where)].astype(jnp.float32) for t, at_ in terms]
                ref[(*lead, *where)] = functools.reduce(lambda a, b: a + b, parts).astype(ref.dtype)

        walk(shape, body)

    def stage(k, q):
        which, layer, shape, slot = jobs[q]
        r1, r2, q1, q2, oc, ob, mb, vb, wb, wn = held[shape]
        _, index = halves(shape)
        if k == 0:
            start(q, S1)
            start(q, S2A)
            for c, d in each:
                own(q, c, d, False).start()
                own(q, c, d, True).start()
        elif k == 1:
            arrived(q, S1)
            taken(local.at[q % TURNS, 0], amount(q, 8))
            for c, d in each:

                @pl.loop(0, side)
                def _(j, c=c, d=d):
                    there = (slot, c, d, j)
                    add(shape, ((r1, there), ((r1, there), (ob, (slot % 2, c, d, j)))))

                copy(q, c, d, S2B).start()
        elif k == 2:
            arrived(q, S2A)
            for c in range(2):
                s = place(c)[1]
                for h, j in ((0, at(s, 2)), (1, at(s, 2)), (1, at(s, 1)), (0, at(s, -1))):
                    here = (slot, c, h, j)
                    add(shape, ((oc, here), ((oc, here), (r2, (slot, c, 0, h, j)), (r2, (slot, c, 1, h, j)))))
            start(q, T1)
            start(q, T2A)
        elif k == 3:
            if slot >= 2:
                taken(stored.at[kinds.index(shape), slot % 2], amount(q, 4))
            for one in state(q):
                one.start()
            arrived(q, T1)
            for c, d in each:
                s = place(c)[1]
                j = at(s, signs[d])
                here = (slot, c, d)
                add(shape, ((q1, here), ((oc, (*here, j)), (r2, (slot, c, 0, d, j)), (r2, (slot, c, 1, d, j)), (q1, here))))
                copy(q, c, d, T2B).start()
        elif k == 4:
            arrived(q, T2A)
            taken(local.at[q % TURNS, 1], amount(q, 4))
            taken(local.at[q % TURNS, 2], wb.at[slot % 2])
            for c in range(2):
                s = place(c)[1]
                for h in range(2):
                    terms = [(oc, (slot, c, h, s))] + [(r2, (slot, c, d, h, s)) for d in range(2)] + [(q2, (slot, c, d, h)) for d in range(2)]
                    quarter = index(2 * c + h)
                    offsets = [x.start if isinstance(x, pl.Slice) else 0 for x in quarter]
                    half = [x.start if isinstance(x, pl.Slice) else 0 for x in index(h)]

                    def body(where, c=c, h=h, terms=terms, offsets=offsets, half=half):
                        def shifted(by):
                            full = []
                            for w, size, o in zip(where, halves(shape)[0], by, strict=True):
                                full.append(pl.ds(o, size) if isinstance(w, slice) else pl.ds(o + w.start, w.size))
                            return tuple(full)

                        g = functools.reduce(lambda a, b: a + b, [t[(*lead, *where)].astype(jnp.float32) for t, lead in terms])
                        g = g.astype(jnp.bfloat16).astype(jnp.float32)
                        there = (slot % 2, *shifted(offsets))
                        w = wb[there].astype(jnp.float32)
                        m = 0.9 * mb[there] + 0.1 * g
                        v = 0.95 * vb[there] + 0.05 * g * g
                        mb[there] = m
                        vb[there] = v
                        new = w - 0.02 * (m * lax.rsqrt(v + 1e-8) + 0.1 * w)
                        wn[(slot, c, *shifted(half))] = new.astype(jnp.bfloat16)

                    walk(shape, body)
                for d in range(2):
                    copy(q, c, d, A1).start()
                weight(q, c).start()
            for one in moments(q):
                one.start()
        elif k == 5:
            arrived(q, A1)
            start(q, A1F)
        elif k == 6:
            taken(local.at[q % TURNS, 3], wn.at[slot])
            arrived(q, A1F)
            start(q, A2P)
            start(q, A2)
        else:
            arrived(q, A2)

    for t in range(len(jobs) + STAGES - 1):
        for k in range(STAGES):
            if 0 <= t - k < len(jobs):
                stage(k, t - k)

    for q, (_, _, shape, slot) in enumerate(jobs):
        if slot + 2 >= seen[shape]:
            taken(stored.at[kinds.index(shape), slot % 2], amount(q, 4))
        if slot + 1 == seen[shape]:
            for i, quarters in enumerate((8, 8, 2, 8)):
                taken(send.at[kinds.index(shape), i], amount(q, quarters * seen[shape]))


def step_kernel(side, layers, shapes, terms, weights, m, v):
    scratch = []
    for shape in dict.fromkeys(shapes):
        count = layers * shapes.count(shape)
        quarter, _ = halves(shape)
        both = (quarter[0] * 2, quarter[1]) if quarter[1] == shape[1] else (quarter[0], quarter[1] * 2)
        scratch += [
            pltpu.VMEM((count, 2, 2, side, *quarter), jnp.bfloat16),
            pltpu.VMEM((count, 2, 2, 2, side, *quarter), jnp.bfloat16),
            pltpu.VMEM((count, 2, 2, *quarter), jnp.bfloat16),
            pltpu.VMEM((count, 2, 2, 2, *quarter), jnp.bfloat16),
            pltpu.VMEM((count, 2, 2, side, *quarter), jnp.bfloat16),
            pltpu.VMEM((2, 2, 2, side, *quarter), jnp.bfloat16),
            pltpu.VMEM((2, *shape), jnp.float32),
            pltpu.VMEM((2, *shape), jnp.float32),
            pltpu.VMEM((2, *shape), jnp.bfloat16),
            pltpu.VMEM((count, 2, *both), jnp.bfloat16),
        ]
    jobs = layers * len(shapes)
    order, groups = ordered(layers, shapes)
    passed = [(len(group), side, *halves(shapes[order[group[0]][0]])[0]) for group in groups for _ in range(4)]
    anywhere = pl.BlockSpec(memory_space=pl.ANY)
    outs = pl.pallas_call(
        functools.partial(kernel, side, layers, shapes),
        out_shape=[jax.ShapeDtypeStruct(w.shape, jnp.bfloat16) for w in weights]
        + [jax.ShapeDtypeStruct(one.shape, jnp.float32) for one in (*m, *v)]
        + [jax.ShapeDtypeStruct(one, jnp.bfloat16) for one in passed],
        in_specs=[anywhere] * (4 * len(shapes)),
        out_specs=[anywhere] * (3 * len(shapes) + len(passed)),
        scratch_shapes=scratch
        + [
            pltpu.SemaphoreType.DMA((len(set(shapes)), 4)),
            pltpu.SemaphoreType.DMA((jobs, 7)),
            pltpu.SemaphoreType.DMA((TURNS, 4)),
            pltpu.SemaphoreType.DMA((len(set(shapes)), 2)),
        ],
        compiler_params=pltpu.CompilerParams(collective_id=0, has_side_effects=True, vmem_limit_bytes=67_043_328),
        name="step",
    )(*terms, *weights, *m, *v)
    return outs[: -len(passed)], outs[-len(passed) :]


def move(moves, slots):
    plan, turns = [], {}
    for src, dst, name in moves:
        buffer, inward, outward = slots[name]
        turn = turns.setdefault(name, [])
        n = len(turn)
        at = n % buffer.shape[0]
        before = turn[n - buffer.shape[0]] if n >= buffer.shape[0] else None
        turn.append(len(plan))
        into = functools.partial(pltpu.make_async_copy, src, buffer.at[at], inward.at[at])
        out_of = functools.partial(pltpu.make_async_copy, buffer.at[at], dst, outward.at[at])
        plan.append((into, out_of, before))
    done = set()
    ahead = 0
    for i in range(len(plan)):
        while ahead < len(plan) and (plan[ahead][2] is None or plan[ahead][2] < i - 2 or ahead == i):
            fetch, _, before = plan[ahead]
            if before is not None:
                plan[before][1]().wait()
                done.add(before)
            fetch().start()
            ahead += 1
        plan[i][0]().wait()
        plan[i][1]().start()
    for i in range(len(plan)):
        if i not in done:
            plan[i][1]().wait()


def chunk(ref, layer, c, h, i, shape):
    quarter = halves(shape)[1](2 * c + h)
    return ref.at[(layer, i, slice(None), *quarter)] if c == 0 else ref.at[(layer, slice(None), i, *quarter)]


def position(side):
    me = lax.axis_index("dp")
    return lax.div(me, side), lax.rem(me, side)


def settle(side, layers, shapes, *refs):
    n = len(shapes)
    order, groups = ordered(layers, shapes)
    handing = 4 * len(groups)
    temps, passed, news = refs[: 3 * n], refs[3 * n : 3 * n + handing], refs[3 * n + handing : 6 * n + handing]
    slots = refs[6 * n + handing :]
    kinds = list(dict.fromkeys(shapes))
    names = {(a, k): slots[6 * i + 3 * j : 6 * i + 3 * j + 3] for i, k in enumerate(kinds) for j, a in enumerate(("moment", "part"))}
    xy = position(side)
    moves = []
    for i in range(n, 3 * n):
        for layer in range(layers):
            moves.append((temps[i].at[layer], news[i].at[layer], ("moment", shapes[i % n])))
    for q, (which, layer) in enumerate(order):
        for c in range(2):
            for h in range(2):
                for by in (0, 1, side - 1):
                    there = (layer, c, h, lax.rem(xy[c] + by, side), shapes[which])
                    src = handed(passed, groups, q, c, h) if by == (side - 1, 1)[h] else chunk(temps[which], *there)
                    moves.append((src, chunk(news[which], *there), ("part", shapes[which])))
    move(moves, names)


def place(side, layers, shapes, jobs, weights, ordering, *refs):
    n = len(weights)
    came, news, sem = refs[n : n + 4], refs[n + 4 + ordering : 2 * n + 4 + ordering], refs[-1]
    xy = position(side)
    copies = []
    for turn, (which, layer) in enumerate(jobs):
        for c in range(2):
            for h in range(2):
                src = came[2 * c + h].at[turn]
                there = (layer, c, h, lax.rem(xy[c] + 2, side), shapes[which])
                copies.append(pltpu.make_async_copy(src, chunk(news[weights.index(which)], *there), sem.at[len(copies)]))
    for one in copies:
        one.start()
    for one in copies:
        one.wait()


def solution(mesh):
    side = math.isqrt(mesh.shape["dp"])

    def step(*arrays):
        terms, weights, m, v = (arrays[i : i + 3] for i in (0, 3, 6, 9))
        shapes = tuple(one.shape[1:] for one in m)
        layers = m[0].shape[0]
        split = [(layers, side, side, *shape) for shape in shapes]
        temps, passed = step_kernel(
            side,
            layers,
            shapes,
            [t[0].reshape(s) for t, s in zip(terms, split, strict=True)],
            [w.reshape(s) for w, s in zip(weights, split, strict=True)],
            m,
            v,
        )
        rings = []
        for c in range(2):
            for by in (1, -1):
                ring = []
                for i in range(side):
                    for j in range(side):
                        to = ((i + by) % side, j) if c == 0 else (i, (j + by) % side)
                        ring.append((i * side + j, to[0] * side + to[1]))
                rings.append(ring)
        came = [lax.ppermute(one, "dp", rings[i % 4]) for i, one in enumerate(passed)]
        anywhere = pl.BlockSpec(memory_space=pl.ANY)

        def slots(count, shape, dtype):
            return [pltpu.VMEM((count, *shape), dtype), pltpu.SemaphoreType.DMA((count,)), pltpu.SemaphoreType.DMA((count,))]

        room = []
        for shape in dict.fromkeys(shapes):
            room += slots(8, shape, jnp.float32) + slots(16, (side, *halves(shape)[0]), jnp.bfloat16)
        bytes_moved = 2 * sum(one.size * one.dtype.itemsize for one in temps)
        new = list(pl.pallas_call(
            functools.partial(settle, side, layers, shapes),
            out_shape=[jax.ShapeDtypeStruct(one.shape, one.dtype) for one in temps],
            in_specs=[anywhere] * (len(temps) + len(passed)),
            out_specs=[anywhere] * len(temps),
            scratch_shapes=room,
            compiler_params=pltpu.CompilerParams(vmem_limit_bytes=SETTLE_VMEM),
            cost_estimate=pl.CostEstimate(flops=10**9, bytes_accessed=bytes_moved, transcendentals=0),
            name="settle",
        )(*temps, *passed))
        order, groups = ordered(layers, shapes)
        before = []
        for i, group in enumerate(groups):
            jobs = [order[q] for q in group]
            to = list(dict.fromkeys(which for which, _ in jobs))
            *last, after = pl.pallas_call(
                functools.partial(place, side, layers, shapes, jobs, to, len(before)),
                out_shape=[jax.ShapeDtypeStruct(new[w].shape, new[w].dtype) for w in to] + [jax.ShapeDtypeStruct((8, 128), jnp.float32)],
                in_specs=[anywhere] * (len(to) + 4 + len(before)),
                out_specs=[anywhere] * (len(to) + 1),
                scratch_shapes=[pltpu.SemaphoreType.DMA((4 * len(jobs),))],
                input_output_aliases={w: w for w in range(len(to))},
                compiler_params=pltpu.CompilerParams(vmem_limit_bytes=PLACE_VMEM),
                cost_estimate=pl.CostEstimate(flops=10**8, bytes_accessed=10**6, transcendentals=0),
                name=f"place_{i}",
            )(*[new[w] for w in to], *came[4 * i : 4 * i + 4], *before)
            before = [after]
            for w, one in zip(to, last, strict=True):
                new[w] = one
        return (*(one.reshape(w.shape) for one, w in zip(new[:3], weights, strict=True)), *new[3:])

    all_of, cut = P(None, None, None), P(None, "dp", None)
    return jax.shard_map(
        step,
        mesh=mesh,
        in_specs=(P(("rep", "dp"), None, None, None),) * 3 + (all_of,) * 3 + (cut,) * 6,
        out_specs=(P("rep", None, None),) * 3 + (P("rep", "dp", None),) * 6,
        check_vma=False,
    )
```
